32 devices in a mesh: rep: 8 (over y, x, core), tp: 4 (over z).
Axes of the slice: x: 2, y: 2, z: 4, core: 2. Of those that a mesh axis runs over, the one named last changes fastest.
Arguments:
- states: bfloat16 [4, 32, 8192], P(None, 'rep'), may hold values from -6 to 6
- norm_gain: float32 [8192], replicated, may hold values from 0.1 to 1.9
- w_query: bfloat16 [8192, 8192], P(('rep', 'tp')), may hold values from -0.0625 to 0.0625
- w_key: bfloat16 [8192, 1024], P(('rep', 'tp')), may hold values from -0.0625 to 0.0625
- w_value: bfloat16 [8192, 1024], P(('rep', 'tp')), may hold values from -0.0625 to 0.0625
- w_out: bfloat16 [8192, 8192], P(None, ('rep', 'tp')), may hold values from -0.0625 to 0.0625
- bias_query: bfloat16 [8192], P('tp'), may hold values from -4 to 4
- bias_key: bfloat16 [1024], P('tp'), may hold values from -4 to 4
- bias_value: bfloat16 [1024], P('tp'), may hold values from -4 to 4
- key_cache: bfloat16 [32, 8, 4096, 128], P('rep', 'tp'), may hold values from -120 to 120
- value_cache: bfloat16 [32, 8, 4096, 128], P('rep', 'tp'), may hold values from -6 to 6
- lengths: int32 [32], P('rep'), may hold values from 1 to 4096, as said below
Outputs:
- mixed: bfloat16 [4, 32, 8192], P(None, 'rep', 'tp')
The draws below stay inside these ranges and needn't reach their ends.
Inputs may be any that keep to these rules, and one draw needn't show every extreme that they name: `lengths`: each row's number of live cached positions; some row has exactly 4096.
All inputs are finite; a program needn't handle non-finite values.
Results may differ from the reference program's by a relative error of at most 0.0084.
Values may be sent and summed in bfloat16 or wider, within the bound.
A program may use at most 128 MiB of HBM per device.

```python
import jax
import jax.numpy as jnp
from jax import lax

D = 8192
KVH = 8
HS = 128
CTX = 4096
STEPS = 4
KVD = 1024
ROWS = 32


def draw_key_cache(key, part):
    shape = (ROWS, KVH, CTX, HS)
    base = jnp.clip(jax.random.normal(key, shape, jnp.float32), -6.0, 6.0)
    return base.astype(jnp.bfloat16)


def draw_lengths(key, part):
    values = jax.random.randint(key, (ROWS,), 1, CTX + 1)
    chosen = jax.random.randint(jax.random.fold_in(key, 3), (), 0, ROWS)
    return jnp.where(jnp.arange(ROWS) == chosen, CTX, values).astype(jnp.int32)


def steps_of(own_key, shape, pieces, smallest, largest):
    def one(position, blocks):
        steps = jax.random.uniform(jax.random.fold_in(jax.random.fold_in(own_key, 6), position), (blocks,), jnp.float32, smallest / len(pieces), largest / len(pieces))
        return jnp.repeat(jnp.exp(steps), shape[position] // blocks).reshape((-1,) + (1,) * (len(shape) - position - 1))

    loudness = one(*pieces[0])
    for cut in pieces[1:]:
        loudness = loudness * one(*cut)
    return loudness


def noise(stream_key, extent, spread, limit, split=(), kind=jnp.bfloat16):
    loudness = steps_of(stream_key, extent, split, -0.22, 0.18) if split else 1.0
    result = jax.random.normal(stream_key, extent, jnp.float32) * spread * loudness
    return jnp.minimum(jnp.maximum(result, -limit), limit).astype(kind)


def setup_inputs(seed: int = 0) -> dict:
    streams_of = jax.random.split(jax.random.key(seed), 13)
    return {
        "states": noise(streams_of[0], (STEPS, ROWS, D), 1.0, 6.0, ((1, 8),)),
        "norm_gain": jnp.clip(1.0 + 0.18 * jax.random.normal(streams_of[1], (D,), jnp.float32), 0.1, 1.9),
        "w_query": noise(streams_of[2], (D, D), D ** -0.5, 0.0625, ((0, 32),)),
        "w_key": noise(streams_of[3], (D, KVD), D ** -0.5, 0.0625, ((0, 32),)),
        "w_value": noise(streams_of[4], (D, KVD), D ** -0.5, 0.0625, ((0, 32),)),
        "w_out": noise(streams_of[5], (D, D), D ** -0.5, 0.0625, ((1, 32),)),
        "bias_query": noise(streams_of[6], (D,), 1.0, 4.0, ((0, 4),)),
        "bias_key": noise(streams_of[7], (KVD,), 1.0, 4.0, ((0, 4),)),
        "bias_value": noise(streams_of[8], (KVD,), 1.0, 4.0, ((0, 4),)),
        "key_cache": draw_key_cache(jax.random.fold_in(streams_of[12], 71), 0),
        "value_cache": noise(streams_of[10], (ROWS, KVH, CTX, HS), 1.0, 6.0, ((0, 8), (1, 4))),
        "lengths": draw_lengths(jax.random.fold_in(streams_of[12], 71), 0),
    }


THETA = 1000000.0
EPS = 1e-06

def rotate(vectors, positions, head_size):
    half = head_size // 2
    freqs = THETA ** (-jnp.arange(half, dtype=jnp.float32) * 2.0 / head_size)
    angles = positions.astype(jnp.float32)[..., None, None] * freqs
    first = vectors[..., :half]
    second = vectors[..., half:]
    cosine = jnp.cos(angles)
    sine = jnp.sin(angles)
    return jnp.concatenate([first * cosine - second * sine, second * cosine + first * sine], axis=-1)

def reference(states, norm_gain, w_query, w_key, w_value, w_out, bias_query, bias_key, bias_value, key_cache, value_cache, lengths):
    steps, rows, width = states.shape
    heads_kv = key_cache.shape[1]
    head_size = key_cache.shape[3]
    heads_q = width // head_size
    group = heads_q // heads_kv
    flat = states.reshape(steps * rows, width).astype(jnp.float32)
    factor = lax.rsqrt(lax.optimization_barrier(jnp.mean(flat * flat, axis=-1, keepdims=True)) + EPS)
    normed = (flat * factor * norm_gain.astype(jnp.float32)).astype(jnp.bfloat16)
    query = jnp.dot(normed, w_query, preferred_element_type=jnp.float32) + bias_query.astype(jnp.float32)
    keys = jnp.dot(normed, w_key, preferred_element_type=jnp.float32) + bias_key.astype(jnp.float32)
    values = jnp.dot(normed, w_value, preferred_element_type=jnp.float32) + bias_value.astype(jnp.float32)
    positions = lengths.astype(jnp.int32)[None, :] + jnp.arange(steps, dtype=jnp.int32)[:, None]
    query = rotate(query.reshape(steps, rows, heads_q, head_size), positions, head_size).astype(jnp.bfloat16)
    keys = rotate(keys.reshape(steps, rows, heads_kv, head_size), positions, head_size).astype(jnp.bfloat16)
    values = values.reshape(steps, rows, heads_kv, head_size).astype(jnp.bfloat16)
    scale = 1.0 / head_size ** 0.5
    count = steps * group

    def one_row(items):
        row_query, row_keys, row_values, cache_k, cache_v, length = items
        grouped = row_query.reshape(steps, heads_kv, group, head_size).transpose(1, 0, 2, 3)
        grouped = grouped.reshape(heads_kv, count, head_size).astype(jnp.float32)
        old_scores = jnp.einsum('kqh,kch->kqc', grouped, cache_k.astype(jnp.float32)) * scale
        old_valid = (jnp.arange(cache_k.shape[1], dtype=jnp.int32) < length)[None, None, :]
        new_scores = jnp.einsum('kqh,jkh->kqj', grouped, row_keys.astype(jnp.float32)) * scale
        rank = jnp.arange(count, dtype=jnp.int32) // group
        new_valid = (jnp.arange(steps, dtype=jnp.int32)[None, :] <= rank[:, None])[None, :, :]
        scores = jnp.concatenate([old_scores, new_scores], axis=-1)
        valid = jnp.concatenate([jnp.broadcast_to(old_valid, old_scores.shape), jnp.broadcast_to(new_valid, new_scores.shape)], axis=-1)
        scores = jnp.where(valid, scores, -1e+30)
        top = lax.optimization_barrier(jnp.max(scores, axis=-1, keepdims=True))
        weights = jnp.where(valid, jnp.exp(scores - top), 0.0)
        total = lax.optimization_barrier(jnp.sum(weights, axis=-1, keepdims=True))
        rounded = weights.astype(jnp.bfloat16).astype(jnp.float32)
        every_value = jnp.concatenate([cache_v, row_values.transpose(1, 0, 2)], axis=1).astype(jnp.float32)
        attended = jnp.einsum('kqc,kch->kqh', rounded, every_value) / total
        attended = attended.reshape(heads_kv, steps, group, head_size).transpose(1, 0, 2, 3)
        return attended.reshape(steps, width).astype(jnp.bfloat16)
    attended = lax.map(one_row, (query.transpose(1, 0, 2, 3), keys.transpose(1, 0, 2, 3), values.transpose(1, 0, 2, 3), key_cache, value_cache, lengths.astype(jnp.int32)))
    attended = attended.transpose(1, 0, 2).reshape(steps * rows, width)
    mixed = flat + jnp.dot(attended, w_out, preferred_element_type=jnp.float32)
    return mixed.astype(jnp.bfloat16).reshape(steps, rows, width)
```

```python
import functools

import jax
import jax.numpy as jnp
import numpy as np
from jax import lax
from jax.experimental import pallas as pl
from jax.experimental.pallas import tpu as pltpu
from jax.sharding import PartitionSpec as P

THETA = 1000000.0
EPS = 1e-06
MESH = pl.DeviceIdType.MESH
BLK = 1024
TILE = 256
LOG2E = 1.4426950408889634
CONTRACT = (((1,), (1,)), ((), ()))


def remote(src, dst, send, recv, device):
    return pltpu.make_async_remote_copy(
        src_ref=src, dst_ref=dst, send_sem=send, recv_sem=recv,
        device_id=device, device_id_type=MESH,
    )


def flip(index, mask, size):
    result, bit = 0, 1
    while bit < size:
        digit = lax.rem(index // bit, 2)
        result = result + bit * (1 - digit if mask & bit else digit)
        bit *= 2
    return result


def block_kernel(
    R, T, direct,
    len_ref, freq_ref, x_ref, send_ref, gain_ref, bq_ref, bk_ref, bv_ref,
    wq_ref, wk_ref, wv_ref, wo_ref, kc_ref, vc_ref,
    out_ref,
    xs, xf, xg, ssq, wbuf, wobuf, kbuf, vbuf,
    own, send0, recv0, send1, recv1, send2, recv2, send3, recv3,
    joined, qbuf, knew, vnew, sbuf, abuf, att, acc, obuf,
    wsem, wosem, ksem, vsem, lsem, xsend, xrecv,
    s0s, s0r, s1s, s1r, s2s, s2r, s3s, s3r,
    zsend, zrecv, csend, crecv, psend, precv, osend, orecv, ready,
):
    r, t = lax.axis_index("rep"), lax.axis_index("tp")
    half, X = R // 2, 2
    Y = half // X
    c, q = lax.rem(r, 2), r // 2
    x, y = lax.rem(q, X), q // X
    steps, rows, width = x_ref.shape
    count = steps * rows
    depth = wq_ref.shape[0]
    G = kc_ref.shape[1]
    context, hs = kc_ref.shape[2], kc_ref.shape[3]
    gq = wq_ref.shape[1] // (T * G)
    gh = gq // hs
    cw = gq + 2 * hs
    N = G * T
    bf, f32 = jnp.bfloat16, jnp.float32

    def dev(yy, xx, cc):
        return ((yy * X + xx) * 2 + cc, t)

    partner = dev(y, x, 1 - c)

    def target(j):
        return flip(t, T - 1 - j, T)

    def weights(n):
        g, d = n // T, target(n % T)
        group = []
        for i, (ref, size, place) in enumerate(
            ((wq_ref, gq, 0), (wk_ref, hs, gq), (wv_ref, hs, gq + hs))
        ):
            start = pl.multiple_of((d * G + g) * size, size)
            group.append(
                pltpu.make_async_copy(
                    ref.at[:, pl.ds(start, size)],
                    wbuf.at[n, :, pl.ds(place, size)],
                    wsem.at[n, i],
                )
            )
        return group

    loads = [weights(n) for n in range(N)]
    for group in loads:
        for copy in group:
            copy.start()

    barrier = pltpu.get_barrier_semaphore()
    for d in range(1, R):
        pl.semaphore_signal(
            barrier, inc=1, device_id=(lax.rem(r + d, R), t), device_id_type=MESH
        )
    for d in range(1, T):
        pl.semaphore_signal(
            barrier, inc=1, device_id=(r, lax.rem(t + d, T)), device_id_type=MESH
        )
    pl.semaphore_wait(barrier, R + T - 2)

    sends = []

    def begin(copy):
        copy.start()
        sends.append(copy)

    def features(peer):
        if direct:
            start = pl.multiple_of((peer * T + t) * depth, depth)
            return x_ref.at[:, :, pl.ds(start, depth)]
        return send_ref.at[peer]

    def slot_of(peer):
        qq = peer // 2
        return xs.at[lax.rem(peer, 2), qq // X, lax.rem(qq, X)]

    for d in range(1, R):
        peer = lax.rem(r + d, R)
        begin(remote(features(peer), slot_of(r), xsend.at[d], xrecv.at[d], (peer, t)))
    for d in range(1, T):
        pl.semaphore_signal(
            ready, inc=1, device_id=(r, lax.rem(t + d, T)), device_id_type=MESH
        )

    caches = {}
    for h in range(G):
        for b in range(rows):
            caches[h, b] = (
                pltpu.make_async_copy(kc_ref.at[b, h], kbuf.at[b, h], ksem.at[b, h]),
                pltpu.make_async_copy(vc_ref.at[b, h], vbuf.at[b, h], vsem.at[b, h]),
            )
    outs = [
        pltpu.make_async_copy(wo_ref.at[pl.ds(k * gq, gq), :], wobuf.at[k], wosem.at[k])
        for k in range(N)
    ]

    for i in range(steps):
        value = x_ref[i].astype(f32)
        square = jnp.sum(value * value, axis=-1, keepdims=True)
        ssq[pl.ds(i * rows, rows), :] = jnp.broadcast_to(square, (rows, hs))
    factor = lax.rsqrt(ssq[...] * (1.0 / width) + EPS)
    rank = lax.broadcasted_iota(jnp.int32, (count, hs), 0)
    spot = lax.broadcasted_iota(jnp.int32, (count, hs), 1)
    position = rank // rows
    for b in range(rows):
        position = position + jnp.where(lax.rem(rank, rows) == b, len_ref[b], 0)
    angle = position.astype(f32) * freq_ref[...]
    cosine = jnp.cos(angle)
    sine = jnp.where(spot < hs // 2, -1.0, 1.0) * jnp.sin(angle)

    for d in range(1, R):
        source = lax.rem(r + R - d, R)
        slot = slot_of(source)
        remote(slot, slot, xsend.at[d], xrecv.at[d], (source, t)).wait_recv()
    if direct:
        here = x_ref[:, :, pl.ds(pl.multiple_of((r * T + t) * depth, depth), depth)]
        gain = gain_ref[:, pl.ds(pl.multiple_of((r * T + t) * depth, depth), depth)]
    else:
        here = send_ref[r]
        gain = gain_ref[...]
    xs[c, y, x] = here
    for k in range(2):
        cc = 1 - c if k == 0 else c
        for yy in range(Y):
            for xx in range(X):
                for i in range(steps):
                    at = (((k * Y + yy) * X + xx) * steps + i) * rows
                    xf[pl.ds(at, rows), :] = xs[cc, yy, xx, i].astype(f32)
    xg[...] = (xf[...] * gain).astype(bf)

    def stage0(n):
        for copy in loads[n]:
            copy.wait()

        def tile(i, _):
            cols = pl.ds(pl.multiple_of(i * TILE, TILE), TILE)
            part = jnp.dot(xg[...], wbuf[n, :, cols], preferred_element_type=f32)
            part = part.reshape(2, Y, X, count, TILE)
            send0[n, :, :, :, cols] = part[0].astype(bf)
            own[n, :, :, :, cols] = part[1]
            return 0

        lax.fori_loop(0, cw // TILE, tile, 0)
        begin(remote(send0.at[n], recv0.at[n], s0s.at[n], s0r.at[n], partner))

    def x_first(n):
        return n % 2 == 0

    def stage1(n):
        remote(send0.at[n], recv0.at[n], s0s.at[n], s0r.at[n], partner).wait_recv()
        if x_first(n):
            for yy in range(Y):
                send1[n, yy] = (own[n, yy, 1 - x] + recv0[n, yy, 1 - x].astype(f32)).astype(bf)
            piece = pl.ds(0, Y)
            begin(remote(
                send1.at[n, piece], recv1.at[n, piece], s1s.at[n, 0], s1r.at[n, 0],
                dev(y, 1 - x, c),
            ))
            for yy in range(Y):
                own[n, yy, x] += recv0[n, yy, x].astype(f32)
        else:
            for d in range(1, Y):
                yy = lax.rem(y + d, Y)
                piece = pl.ds((d - 1) * X, X)
                send1[n, piece] = (own[n, yy] + recv0[n, yy].astype(f32)).astype(bf)
                begin(remote(
                    send1.at[n, piece], recv1.at[n, piece], s1s.at[n, d - 1], s1r.at[n, d - 1],
                    dev(yy, x, c),
                ))
            own[n, y] += recv0[n, y].astype(f32)

    def stage2(n):
        if x_first(n):
            piece = pl.ds(0, Y)
            remote(
                send1.at[n, piece], recv1.at[n, piece], s1s.at[n, 0], s1r.at[n, 0], partner
            ).wait_recv()
            for d in range(1, Y):
                yy = lax.rem(y + d, Y)
                send2[n, d - 1] = (own[n, yy, x] + recv1[n, yy].astype(f32)).astype(bf)
                begin(remote(
                    send2.at[n, d - 1], recv2.at[n, d - 1], s2s.at[n, d - 1], s2r.at[n, d - 1],
                    dev(yy, x, c),
                ))
            own[n, y, x] += recv1[n, y].astype(f32)
        else:
            for d in range(1, Y):
                piece = pl.ds((d - 1) * X, X)
                remote(
                    send1.at[n, piece], recv1.at[n, piece], s1s.at[n, d - 1], s1r.at[n, d - 1],
                    partner,
                ).wait_recv()
            away, keep = own[n, y, 1 - x], own[n, y, x]
            for d in range(1, Y):
                away += recv1[n, (d - 1) * X + 1 - x].astype(f32)
                keep += recv1[n, (d - 1) * X + x].astype(f32)
            send2[n, 0] = away.astype(bf)
            begin(remote(
                send2.at[n, 0], recv2.at[n, 0], s2s.at[n, 0], s2r.at[n, 0], dev(y, 1 - x, c)
            ))
            own[n, y, x] = keep

    def stage3(n):
        g, j = n // T, n % T
        total = own[n, y, x]
        for d in range(Y - 1 if x_first(n) else 1):
            slot = recv2.at[n, d]
            remote(slot, slot, s2s.at[n, d], s2r.at[n, d], partner).wait_recv()
            total += slot[...].astype(f32)
        if j < T - 1:
            send3[n] = total.astype(bf)
            begin(remote(
                send3.at[n], recv3.at[n], s3s.at[n], s3r.at[n], (r, target(j))
            ))
        else:
            joined[g] = total

    def turn(value):
        return value * cosine + pltpu.roll(value, hs // 2, 1) * sine

    def stage4(g):
        for j in range(T - 1):
            slot = recv3.at[g * T + j]
            remote(slot, slot, s3s.at[g * T + j], s3r.at[g * T + j], partner).wait_recv()
            joined[g] += slot[...].astype(f32)
        for k in range(gh):
            bias = bq_ref[pl.ds(g * gh + k, 1), :].astype(f32)
            value = joined[g, :, pl.ds(k * hs, hs)] * factor + bias
            qbuf[g, pl.ds(k * count, count), :] = turn(value) * (LOG2E / hs**0.5)
        bias = bk_ref[pl.ds(g, 1), :].astype(f32)
        knew[g] = turn(joined[g, :, pl.ds(gq, hs)] * factor + bias).astype(bf)
        bias = bv_ref[pl.ds(g, 1), :].astype(f32)
        vnew[g] = (joined[g, :, pl.ds(gq + hs, hs)] * factor + bias).astype(bf)

    block = min(BLK, context)
    lines = gh * steps

    def unit(g, b):
        for copy in caches[g, b]:
            copy.wait()
        length = len_ref[b]
        qb = qbuf[g, pl.ds(b, lines, stride=rows), :].astype(bf)
        fresh = lax.dot_general(qb, knew[g], CONTRACT, preferred_element_type=f32)
        asker = lax.rem(lax.broadcasted_iota(jnp.int32, (lines, count), 0), steps)
        place = lax.broadcasted_iota(jnp.int32, (lines, count), 1)
        fine = (lax.rem(place, rows) == b) & (place // rows <= asker)
        fresh = jnp.where(fine, fresh, -1e30)
        peak = jnp.max(fresh, axis=-1, keepdims=True)
        tops = None
        for k in range(context // block):
            part = pl.ds(k * block, block)
            scores = lax.dot_general(qb, kbuf[b, g, part, :], CONTRACT, preferred_element_type=f32)
            where = k * block + lax.broadcasted_iota(jnp.int32, (lines, block), 1)
            scores = jnp.where(where < length, scores, -1e30)
            sbuf[b % 2, :, part] = scores
            for s in range(block // hs):
                piece = scores[:, s * hs : (s + 1) * hs]
                tops = piece if tops is None else jnp.maximum(tops, piece)
        peak = jnp.maximum(peak, jnp.max(tops, axis=-1, keepdims=True))
        weights = jnp.exp2(fresh - peak)
        total = jnp.sum(weights, axis=-1, keepdims=True)
        result = jnp.dot(weights.astype(bf), vnew[g], preferred_element_type=f32)
        sums = None
        for k in range(context // block):
            part = pl.ds(k * block, block)
            weights = jnp.exp2(sbuf[b % 2, :, part] - peak)
            for s in range(block // hs):
                piece = weights[:, s * hs : (s + 1) * hs]
                sums = piece if sums is None else sums + piece
            result += jnp.dot(
                weights.astype(bf), vbuf[b, g, part, :], preferred_element_type=f32
            )
        total = total + jnp.sum(sums, axis=-1, keepdims=True)
        abuf[g, pl.ds(b, lines, stride=rows), :] = result / total

    def attend(g):
        for b in range(rows):
            unit(g, b)
        for k in range(gh):
            att[g, t, c, y, x, :, pl.ds(k * hs, hs)] = abuf[g, pl.ds(k * count, count), :].astype(bf)

    peers = [0] + list(range(T - 1, 0, -1))

    def spread(g):
        mine = att.at[g, t, c, y, x]
        for m in range(1, T):
            begin(remote(mine, mine, zsend.at[g, m], zrecv.at[g, m], (r, flip(t, m, T))))
        across(g, 0)

    def across(g, m):
        piece = att.at[g, flip(t, m, T), c, y, x]
        if m:
            remote(piece, piece, zsend.at[g, m], zrecv.at[g, m], partner).wait_recv()
        for e in range(1, half):
            to = lax.rem(q + e, half)
            begin(remote(
                piece, piece, csend.at[g, m, e], crecv.at[g, m, e], (2 * to + c, t)
            ))

    def collect(g, m):
        for e in range(1, half):
            source = lax.rem(q + half - e, half)
            piece = att.at[g, flip(t, m, T), c, source // X, lax.rem(source, X)]
            remote(piece, piece, csend.at[g, m, e], crecv.at[g, m, e], partner).wait_recv()
        whole = att.at[g, flip(t, m, T), c]
        begin(remote(whole, whole, psend.at[g, m], precv.at[g, m], partner))

    def multiply(g, m, first):
        tt = flip(t, m, T)
        other = att.at[g, tt, 1 - c]
        remote(other, other, psend.at[g, m], precv.at[g, m], partner).wait_recv()
        part = jnp.dot(
            att[g, tt].reshape(R * count, gq), wobuf[tt * G + g], preferred_element_type=f32
        )
        if first:
            acc[...] = part
        else:
            acc[...] += part

    for n in range(N):
        stage0(n)
        if n >= 1:
            stage1(n - 1)
    for h in range(G):
        for b in range(rows):
            for copy in caches[h, b]:
                copy.start()
    for copy in outs:
        copy.start()
    stage1(N - 1)
    for n in range(N + 1):
        if n < N:
            stage2(n)
        if n >= 1:
            stage3(n - 1)
    for g in range(G):
        stage4(g)
        attend(g)
        spread(g)
    for g in range(G):
        for m in peers[1:]:
            across(g, m)
    for copy in outs:
        copy.wait()
    for g in range(G):
        for m in peers:
            collect(g, m)
    for g in range(G):
        for m in peers:
            multiply(g, m, g == 0 and m == 0)

    obuf[...] = acc[...].astype(bf).reshape(obuf.shape)
    block_at = r * T + t
    home, slot = block_at // R, lax.rem(block_at, R)
    pl.semaphore_wait(ready, T - 1)
    for d in range(1, R):
        to = lax.rem(r + d, R)
        qq = to // 2
        piece = obuf.at[lax.rem(to, 2), qq // X, lax.rem(qq, X)]
        begin(remote(piece, out_ref.at[slot], osend.at[d], orecv.at[slot], (to, home)))
    mine = obuf.at[c, y, x]

    @pl.when(home == t)
    def _():
        copy = pltpu.make_async_copy(mine, out_ref.at[slot], orecv.at[slot])
        copy.start()

    @pl.when(home != t)
    def _():
        copy = remote(mine, out_ref.at[slot], osend.at[0], orecv.at[slot], (r, home))
        copy.start()
        copy.wait_send()

    for s in range(R):
        piece = out_ref.at[s]
        pltpu.make_async_copy(piece, piece, orecv.at[s]).wait()
    for copy in sends:
        copy.wait_send()


def on_device(
    R, T, states, norm_gain, w_query, w_key, w_value, w_out,
    bias_query, bias_key, bias_value, key_cache, value_cache, lengths,
):
    steps, rows, width = states.shape
    G, context, hs = key_cache.shape[1:]
    count = steps * rows
    depth = w_query.shape[0]
    columns = w_out.shape[1]
    gq = w_query.shape[1] // (T * G)
    gh = gq // hs
    cw = gq + 2 * hs
    N = G * T
    half, X = R // 2, 2
    Y = half // X
    direct = depth % hs == 0
    t = lax.axis_index("tp")
    at = lax.axis_index("rep") * T + t
    bf, f32 = jnp.bfloat16, jnp.float32
    gain = norm_gain.reshape(1, width)
    sent = states
    if not direct:
        gain = lax.dynamic_slice_in_dim(gain, at * depth, depth, 1)
        sent = states.reshape(steps, rows, R, T, depth)
        sent = lax.dynamic_index_in_dim(sent, t, 3, keepdims=False).transpose(2, 0, 1, 3)
    lane = np.arange(hs) % (hs // 2)
    freqs = (np.float32(THETA) ** (-lane.astype(np.float32) * np.float32(2.0) / np.float32(hs)))
    freqs = jnp.asarray(freqs.astype(np.float32).reshape(1, hs))
    smem = pl.BlockSpec(memory_space=pltpu.SMEM)
    vmem = pl.BlockSpec(memory_space=pltpu.VMEM)
    hbm = pl.BlockSpec(memory_space=pl.ANY)
    dma = pltpu.SemaphoreType.DMA
    V = pltpu.VMEM
    k1, k2 = max(Y, (Y - 1) * X), max(Y - 1, 1)
    pieces = pl.pallas_call(
        functools.partial(block_kernel, R, T, direct),
        out_shape=jax.ShapeDtypeStruct((R, count, columns), bf),
        in_specs=[smem] + [vmem] * 7 + [hbm] * 6,
        out_specs=vmem,
        scratch_shapes=[
            V((2, Y, X, steps, rows, depth), bf), V((R * count, depth), f32),
            V((R * count, depth), bf), V((count, hs), f32),
            V((N, depth, cw), bf), V((N, gq, columns), bf),
            V((rows, G, context, hs), bf), V((rows, G, context, hs), bf),
            V((N, Y, X, count, cw), f32),
            V((N, Y, X, count, cw), bf), V((N, Y, X, count, cw), bf),
            V((N, k1, count, cw), bf), V((N, k1, count, cw), bf),
            V((N, k2, count, cw), bf), V((N, k2, count, cw), bf),
            V((N, count, cw), bf), V((N, count, cw), bf),
            V((G, count, cw), f32), V((G, gh * count, hs), f32),
            V((G, count, hs), bf), V((G, count, hs), bf),
            V((2, gh * steps, context), f32), V((G, gh * count, hs), f32),
            V((G, T, 2, Y, X, count, gq), bf), V((R * count, columns), f32),
            V((2, Y, X, count, columns), bf),
            dma((N, 3)), dma((N,)), dma((rows, G)), dma((rows, G)), dma, dma((R,)), dma((R,)),
            dma((N,)), dma((N,)), dma((N, k1)), dma((N, k1)), dma((N, k2)), dma((N, k2)),
            dma((N,)), dma((N,)),
            dma((G, T)), dma((G, T)), dma((G, T, half)), dma((G, T, half)),
            dma((G, T)), dma((G, T)), dma((R,)), dma((R,)), pltpu.SemaphoreType.REGULAR,
        ],
        compiler_params=pltpu.CompilerParams(
            collective_id=0, has_side_effects=True, vmem_limit_bytes=67043328
        ),
        name="block",
    )(
        lengths, freqs, states, sent, gain,
        bias_query.reshape(-1, hs), bias_key.reshape(-1, hs), bias_value.reshape(-1, hs),
        w_query, w_key, w_value, w_out, key_cache, value_cache,
    )
    share = R * columns
    summed = pieces.reshape(R, steps, rows, columns).transpose(1, 2, 0, 3)
    summed = summed.reshape(steps, rows, share).astype(f32)
    residual = lax.dynamic_slice_in_dim(states, t * share, share, 2).astype(f32)
    return (residual + summed).astype(bf)


def solution(mesh):
    return jax.shard_map(
        functools.partial(on_device, mesh.shape["rep"], mesh.shape["tp"]),
        mesh=mesh,
        in_specs=(
            P(None, "rep", None), P(), P(("rep", "tp"), None), P(("rep", "tp"), None),
            P(("rep", "tp"), None), P(None, ("rep", "tp")), P("tp"), P("tp"), P("tp"),
            P("rep", "tp", None, None), P("rep", "tp", None, None), P("rep"),
        ),
        out_specs=P(None, "rep", "tp"),
        check_vma=False,
    )
```

```python
import functools

import jax
import jax.numpy as jnp
import numpy as np
from jax import lax
from jax.experimental import pallas as pl
from jax.experimental.pallas import tpu as pltpu
from jax.sharding import PartitionSpec as P

THETA = 1000000.0
EPS = 1e-06
MESH = pl.DeviceIdType.MESH
BLK = 1024
TILE = 256
VMEM_KIB = 61440
LOG2E = 1.4426950408889634
CONTRACT = (((1,), (1,)), ((), ()))


def remote(src, dst, send, recv, device):
    return pltpu.make_async_remote_copy(
        src_ref=src, dst_ref=dst, send_sem=send, recv_sem=recv,
        device_id=device, device_id_type=MESH,
    )


def flip(index, mask, size):
    result, bit = 0, 1
    while bit < size:
        digit = lax.rem(index // bit, 2)
        result = result + bit * (1 - digit if mask & bit else digit)
        bit *= 2
    return result


def block_kernel(
    R, T, direct,
    len_ref, freq_hbm, x_hbm, send_hbm, gain_hbm, bq_hbm, bk_hbm, bv_hbm,
    wq_ref, wk_ref, wv_ref, wo_ref, kc_ref, vc_ref,
    out_ref,
    freq_ref, x_ref, send_ref, gain_ref, bq_ref, bk_ref, bv_ref, pieces,
    xs, xf, xg, ssq, wbuf, wobuf, kbuf, vbuf,
    own, send0, recv0, send1, recv1, send2, recv2, send3, recv3,
    joined, qbuf, knew, vnew, sbuf, abuf, att, acc, obuf,
    wsem, wosem, ksem, vsem, isem, xsend, xrecv,
    s0s, s0r, s1s, s1r, s2s, s2r, s3s, s3r,
    zsend, zrecv, csend, crecv, wsend, wrecv, osend, orecv, ready,
):
    r, t = lax.axis_index("rep"), lax.axis_index("tp")
    half, X = R // 2, 2
    Y = half // X
    c, q = lax.rem(r, 2), r // 2
    x, y = lax.rem(q, X), q // X
    steps, rows, width = x_ref.shape
    count = steps * rows
    depth = wq_ref.shape[0]
    G = kc_ref.shape[1]
    context, hs = kc_ref.shape[2], kc_ref.shape[3]
    gq = wq_ref.shape[1] // (T * G)
    gh = gq // hs
    cw = gq + 2 * hs
    N = G * T
    columns = wo_ref.shape[1]
    bf, f32 = jnp.bfloat16, jnp.float32

    def dev(yy, xx, cc):
        return ((yy * X + xx) * 2 + cc, t)

    partner = dev(y, x, 1 - c)

    def target(j):
        return flip(t, T - 1 - j, T)

    def weights(n):
        g, d = n // T, target(n % T)
        group = []
        for i, (ref, size, place) in enumerate(
            ((wq_ref, gq, 0), (wk_ref, hs, gq), (wv_ref, hs, gq + hs))
        ):
            start = pl.multiple_of((d * G + g) * size, size)
            group.append(
                pltpu.make_async_copy(
                    ref.at[:, pl.ds(start, size)],
                    wbuf.at[n, :, pl.ds(place, size)],
                    wsem.at[n, i],
                )
            )
        return group

    loads = [weights(n) for n in range(N)]

    barrier = pltpu.get_barrier_semaphore()
    for d in range(1, R):
        pl.semaphore_signal(
            barrier, inc=1, device_id=(lax.rem(r + d, R), t), device_id_type=MESH
        )
    for d in range(1, T):
        pl.semaphore_signal(
            barrier, inc=1, device_id=(r, lax.rem(t + d, T)), device_id_type=MESH
        )
    mine_at = pl.ds(pl.multiple_of((r * T + t) * depth, depth) if direct else 0, depth)
    small = [
        pltpu.make_async_copy(src, dst, isem.at[i])
        for i, (src, dst) in enumerate((
            (x_hbm, x_ref), (gain_hbm.at[:, mine_at], gain_ref), (freq_hbm, freq_ref),
            (bq_hbm, bq_ref), (bk_hbm, bk_ref), (bv_hbm, bv_ref), (send_hbm, send_ref),
        ))
        if direct is False or dst is not send_ref
    ]
    for copy in small:
        copy.start()
    for group in loads:
        for copy in group:
            copy.start()
    small[0].wait()
    if not direct:
        small[-1].wait()
    pl.semaphore_wait(barrier, R + T - 2)

    sends = []

    def begin(copy):
        copy.start()
        sends.append(copy)

    def features(peer):
        if direct:
            start = pl.multiple_of((peer * T + t) * depth, depth)
            return x_ref.at[:, :, pl.ds(start, depth)]
        return send_ref.at[peer]

    def slot_of(peer):
        qq = peer // 2
        return xs.at[lax.rem(peer, 2), qq // X, lax.rem(qq, X)]

    for d in range(1, R):
        peer = lax.rem(r + d, R)
        begin(remote(features(peer), slot_of(r), xsend.at[d], xrecv.at[d], (peer, t)))
    for d in range(1, T):
        pl.semaphore_signal(
            ready, inc=1, device_id=(r, lax.rem(t + d, T)), device_id_type=MESH
        )

    caches = {}
    for h in range(G):
        for b in range(rows):
            caches[h, b] = (
                pltpu.make_async_copy(kc_ref.at[b, h], kbuf.at[b, h], ksem.at[b, h]),
                pltpu.make_async_copy(vc_ref.at[b, h], vbuf.at[b, h], vsem.at[b, h]),
            )
    outs = []
    for k in range(N):
        part = wo_ref.at[pl.ds(k * gq, gq), :]
        outs.append((
            pltpu.make_async_copy(part, wobuf.at[c, k], wosem.at[k]),
            remote(part, wobuf.at[c, k], wsend.at[k], wrecv.at[k], partner),
        ))

    for copy in small[1:6]:
        copy.wait()

    for i in range(steps):
        value = x_ref[i].astype(f32)
        square = jnp.sum(value * value, axis=-1, keepdims=True)
        ssq[pl.ds(i * rows, rows), :] = jnp.broadcast_to(square, (rows, hs))
    factor = lax.rsqrt(ssq[...] * (1.0 / width) + EPS)
    rank = lax.broadcasted_iota(jnp.int32, (count, hs), 0)
    spot = lax.broadcasted_iota(jnp.int32, (count, hs), 1)
    position = rank // rows
    for b in range(rows):
        position = position + jnp.where(lax.rem(rank, rows) == b, len_ref[b], 0)
    angle = position.astype(f32) * freq_ref[...]
    cosine = jnp.cos(angle)
    sine = jnp.where(spot < hs // 2, -1.0, 1.0) * jnp.sin(angle)

    for d in range(1, R):
        source = lax.rem(r + R - d, R)
        slot = slot_of(source)
        remote(slot, slot, xsend.at[d], xrecv.at[d], (source, t)).wait_recv()
    xs[c, y, x] = x_ref[:, :, mine_at] if direct else send_ref[r]
    for k in range(2):
        cc = 1 - c if k == 0 else c
        for yy in range(Y):
            for xx in range(X):
                for i in range(steps):
                    at = (((k * Y + yy) * X + xx) * steps + i) * rows
                    xf[pl.ds(at, rows), :] = xs[cc, yy, xx, i].astype(f32)
    xg[...] = (xf[...] * gain_ref[...]).astype(bf)

    def stage0(n):
        for copy in loads[n]:
            copy.wait()

        for i in range(cw // TILE):
            cols = pl.ds(i * TILE, TILE)
            part = jnp.dot(xg[...], wbuf[n, :, cols], preferred_element_type=f32)
            part = part.reshape(2, Y, X, count, TILE)
            send0[n, :, :, :, cols] = part[0].astype(bf)
            own[n, :, :, :, cols] = part[1]
        begin(remote(send0.at[n], recv0.at[n], s0s.at[n], s0r.at[n], partner))

    def x_first(n):
        return n % 2 == 0

    def stage1(n):
        remote(send0.at[n], recv0.at[n], s0s.at[n], s0r.at[n], partner).wait_recv()
        if x_first(n):
            for yy in range(Y):
                send1[n, yy] = (own[n, yy, 1 - x] + recv0[n, yy, 1 - x].astype(f32)).astype(bf)
            piece = pl.ds(0, Y)
            begin(remote(
                send1.at[n, piece], recv1.at[n, piece], s1s.at[n, 0], s1r.at[n, 0],
                dev(y, 1 - x, c),
            ))
            for yy in range(Y):
                own[n, yy, x] += recv0[n, yy, x].astype(f32)
        else:
            for d in range(1, Y):
                yy = lax.rem(y + d, Y)
                piece = pl.ds((d - 1) * X, X)
                send1[n, piece] = (own[n, yy] + recv0[n, yy].astype(f32)).astype(bf)
                begin(remote(
                    send1.at[n, piece], recv1.at[n, piece], s1s.at[n, d - 1], s1r.at[n, d - 1],
                    dev(yy, x, c),
                ))
            own[n, y] += recv0[n, y].astype(f32)

    def stage2(n):
        if x_first(n):
            piece = pl.ds(0, Y)
            remote(
                send1.at[n, piece], recv1.at[n, piece], s1s.at[n, 0], s1r.at[n, 0], partner
            ).wait_recv()
            for d in range(1, Y):
                yy = lax.rem(y + d, Y)
                send2[n, d - 1] = (own[n, yy, x] + recv1[n, yy].astype(f32)).astype(bf)
                begin(remote(
                    send2.at[n, d - 1], recv2.at[n, d - 1], s2s.at[n, d - 1], s2r.at[n, d - 1],
                    dev(yy, x, c),
                ))
            own[n, y, x] += recv1[n, y].astype(f32)
        else:
            for d in range(1, Y):
                piece = pl.ds((d - 1) * X, X)
                remote(
                    send1.at[n, piece], recv1.at[n, piece], s1s.at[n, d - 1], s1r.at[n, d - 1],
                    partner,
                ).wait_recv()
            away, keep = own[n, y, 1 - x], own[n, y, x]
            for d in range(1, Y):
                away += recv1[n, (d - 1) * X + 1 - x].astype(f32)
                keep += recv1[n, (d - 1) * X + x].astype(f32)
            send2[n, 0] = away.astype(bf)
            begin(remote(
                send2.at[n, 0], recv2.at[n, 0], s2s.at[n, 0], s2r.at[n, 0], dev(y, 1 - x, c)
            ))
            own[n, y, x] = keep

    def stage3(n):
        g, j = n // T, n % T
        total = own[n, y, x]
        for d in range(Y - 1 if x_first(n) else 1):
            slot = recv2.at[n, d]
            remote(slot, slot, s2s.at[n, d], s2r.at[n, d], partner).wait_recv()
            total += slot[...].astype(f32)
        if j < T - 1:
            send3[n] = total.astype(bf)
            begin(remote(
                send3.at[n], recv3.at[n], s3s.at[n], s3r.at[n], (r, target(j))
            ))
        else:
            joined[g] = total

    def turn(value):
        return value * cosine + pltpu.roll(value, hs // 2, 1) * sine

    def stage4(g):
        for j in range(T - 1):
            slot = recv3.at[g * T + j]
            remote(slot, slot, s3s.at[g * T + j], s3r.at[g * T + j], partner).wait_recv()
            joined[g] += slot[...].astype(f32)
        for k in range(gh):
            bias = bq_ref[pl.ds(g * gh + k, 1), :].astype(f32)
            value = joined[g, :, pl.ds(k * hs, hs)] * factor + bias
            qbuf[g, pl.ds(k * count, count), :] = turn(value) * (LOG2E / hs**0.5)
        bias = bk_ref[pl.ds(g, 1), :].astype(f32)
        knew[g] = turn(joined[g, :, pl.ds(gq, hs)] * factor + bias).astype(bf)
        bias = bv_ref[pl.ds(g, 1), :].astype(f32)
        vnew[g] = (joined[g, :, pl.ds(gq + hs, hs)] * factor + bias).astype(bf)

    block = min(BLK, context)
    lines = gh * steps

    def unit(g, b):
        for copy in caches[g, b]:
            copy.wait()
        length = len_ref[b]
        qb = qbuf[g, pl.ds(b, lines, stride=rows), :].astype(bf)
        fresh = lax.dot_general(qb, knew[g], CONTRACT, preferred_element_type=f32)
        asker = lax.rem(lax.broadcasted_iota(jnp.int32, (lines, count), 0), steps)
        place = lax.broadcasted_iota(jnp.int32, (lines, count), 1)
        fine = (lax.rem(place, rows) == b) & (place // rows <= asker)
        fresh = jnp.where(fine, fresh, -1e30)
        peak = jnp.max(fresh, axis=-1, keepdims=True)
        tops = None
        for k in range(context // block):
            part = pl.ds(k * block, block)
            scores = lax.dot_general(qb, kbuf[b, g, part, :], CONTRACT, preferred_element_type=f32)
            where = k * block + lax.broadcasted_iota(jnp.int32, (lines, block), 1)
            scores = jnp.where(where < length, scores, -1e30)
            sbuf[b % 2, :, part] = scores
            for s in range(block // hs):
                piece = scores[:, s * hs : (s + 1) * hs]
                tops = piece if tops is None else jnp.maximum(tops, piece)
        peak = jnp.maximum(peak, jnp.max(tops, axis=-1, keepdims=True))
        weights = jnp.exp2(fresh - peak)
        total = jnp.sum(weights, axis=-1, keepdims=True)
        result = jnp.dot(weights.astype(bf), vnew[g], preferred_element_type=f32)
        sums = None
        for k in range(context // block):
            part = pl.ds(k * block, block)
            weights = jnp.exp2(sbuf[b % 2, :, part] - peak)
            for s in range(block // hs):
                piece = weights[:, s * hs : (s + 1) * hs]
                sums = piece if sums is None else sums + piece
            result += jnp.dot(
                weights.astype(bf), vbuf[b, g, part, :], preferred_element_type=f32
            )
        total = total + jnp.sum(sums, axis=-1, keepdims=True)
        abuf[g, pl.ds(b, lines, stride=rows), :] = result / total

    def finish(g):
        for k in range(gh):
            att[g, t, y, x, :, pl.ds(k * hs, hs)] = abuf[g, pl.ds(k * count, count), :].astype(bf)

    def spread(g):
        mine = att.at[g, t, y, x]
        for m in range(T - 1, 0, -1):
            begin(remote(mine, mine, zsend.at[g, m], zrecv.at[g, m], (r, flip(t, m, T))))
        across(g, 0)

    def plane(g, m, yy, xx, k, to):
        piece = att.at[g, flip(t, m, T), yy, xx]
        return remote(piece, piece, csend.at[g, m, k], crecv.at[g, m, k], to)

    def across(g, m):
        if m:
            piece = att.at[g, flip(t, m, T), y, x]
            remote(piece, piece, zsend.at[g, m], zrecv.at[g, m], partner).wait_recv()
        begin(plane(g, m, y, x, 0, dev(y, 1 - x, c)))
        for d in range(1, Y):
            begin(plane(g, m, y, x, d, dev(lax.rem(y + d, Y), x, c)))

    def relay(g, m):
        if m % 2 == 0:
            plane(g, m, y, 1 - x, 0, partner).wait_recv()
            for d in range(1, Y):
                begin(plane(g, m, y, 1 - x, Y - 1 + d, dev(lax.rem(y + d, Y), x, c)))
        else:
            for d in range(1, Y):
                yy = lax.rem(y + Y - d, Y)
                plane(g, m, yy, x, d, partner).wait_recv()
                begin(plane(g, m, yy, x, Y - 1 + d, dev(y, 1 - x, c)))

    def collect(g, m):
        if m % 2:
            plane(g, m, y, 1 - x, 0, partner).wait_recv()
        for d in range(1, Y):
            yy = lax.rem(y + Y - d, Y)
            if m % 2 == 0:
                plane(g, m, yy, x, d, partner).wait_recv()
            plane(g, m, yy, 1 - x, Y - 1 + d, partner).wait_recv()
    def multiply(g, m, first):
        tt = flip(t, m, T)
        lines = att[g, tt].reshape(half * count, gq)
        for k in range(2):
            part = jnp.dot(lines, wobuf[k, tt * G + g], preferred_element_type=f32)
            if first:
                acc[k] = part
            else:
                acc[k] += part

    early = N // 2
    for n in range(early):
        stage0(n)
    for n in range(early):
        stage1(n)
    for n in range(early, N):
        stage0(n)
    for h in range(G):
        for b in range(rows):
            for copy in caches[h, b]:
                copy.start()
    for copy, swap in outs:
        copy.start()
    for p in range(0, N, 2):
        if p >= 4:
            stage3(p - 4)
            stage3(p - 3)
        stage2(p)
        stage2(p + 1)
        if early + p < N:
            stage1(early + p)
            stage1(early + p + 1)
    for n in range(max(N - 4, 0), N):
        stage3(n)
    for copy, swap in outs:
        begin(swap)
    for g in range(G):
        stage4(g)
        for b in range(rows):
            unit(g, b)
        finish(g)
        spread(g)
    for g in range(G):
        for m in range(1, T):
            across(g, m)
        for m in range(T):
            relay(g, m)
        if g == 0:
            for copy, swap in outs:
                copy.wait()
                swap.wait_recv()
        if g:
            for m in range(T):
                collect(g - 1, m)
                multiply(g - 1, m, g == 1 and m == 0)
    for m in range(T):
        collect(G - 1, m)
        multiply(G - 1, m, G == 1 and m == 0)

    obuf[...] = acc[...].astype(bf).reshape(obuf.shape)
    pl.semaphore_wait(ready, T - 1)
    for k in range(2):
        block_at = (2 * q + k) * T + t
        home, slot = block_at // R, lax.rem(block_at, R)
        for d in range(1, half):
            to = lax.rem(q + d, half)
            begin(remote(
                obuf.at[k, to // X, lax.rem(to, X)], pieces.at[slot], osend.at[k, d],
                orecv.at[slot], (2 * to + c, home),
            ))
        mine = obuf.at[k, y, x]

        @pl.when(home == t)
        def _():
            copy = pltpu.make_async_copy(mine, pieces.at[slot], orecv.at[slot])
            copy.start()

        @pl.when(home != t)
        def _():
            copy = remote(mine, pieces.at[slot], osend.at[k, 0], orecv.at[slot], (r, home))
            copy.start()
            copy.wait_send()

    for s in range(R):
        piece = pieces.at[s]
        pltpu.make_async_copy(piece, piece, orecv.at[s]).wait()
        if direct:
            value = pieces[s].astype(f32)
            cols = pl.ds(s * columns, columns)
            from_x = pl.ds(pl.multiple_of(t * R * columns + s * columns, columns), columns)
            for i in range(steps):
                out_ref[i, :, cols] = (
                    x_ref[i, :, from_x].astype(f32) + value[i * rows : (i + 1) * rows]
                ).astype(bf)
        else:
            out_ref[s] = pieces[s]
    for copy in sends:
        copy.wait_send()


def on_device(
    R, T, states, norm_gain, w_query, w_key, w_value, w_out,
    bias_query, bias_key, bias_value, key_cache, value_cache, lengths,
):
    steps, rows, width = states.shape
    G, context, hs = key_cache.shape[1:]
    count = steps * rows
    depth = w_query.shape[0]
    columns = w_out.shape[1]
    gq = w_query.shape[1] // (T * G)
    gh = gq // hs
    cw = gq + 2 * hs
    N = G * T
    half, X = R // 2, 2
    Y = half // X
    direct = depth % hs == 0 and columns % hs == 0
    share = R * columns
    t = lax.axis_index("tp")
    at = lax.axis_index("rep") * T + t
    bf, f32 = jnp.bfloat16, jnp.float32
    gain = norm_gain.reshape(1, width)
    sent = states
    if not direct:
        gain = lax.dynamic_slice_in_dim(gain, at * depth, depth, 1)
        sent = states.reshape(steps, rows, R, T, depth)
        sent = lax.dynamic_index_in_dim(sent, t, 3, keepdims=False).transpose(2, 0, 1, 3)
    result = (steps, rows, share) if direct else (R, count, columns)
    lane = np.arange(hs) % (hs // 2)
    freqs = (np.float32(THETA) ** (-lane.astype(np.float32) * np.float32(2.0) / np.float32(hs)))
    freqs = jnp.asarray(freqs.astype(np.float32).reshape(1, hs))
    smem = pl.BlockSpec(memory_space=pltpu.SMEM)
    vmem = pl.BlockSpec(memory_space=pltpu.VMEM)
    hbm = pl.BlockSpec(memory_space=pltpu.HBM)
    dma = pltpu.SemaphoreType.DMA
    V = pltpu.VMEM
    k1, k2 = max(Y, (Y - 1) * X), max(Y - 1, 1)
    pieces = pl.pallas_call(
        functools.partial(block_kernel, R, T, direct),
        out_shape=jax.ShapeDtypeStruct(result, bf),
        in_specs=[smem] + [hbm] * 13,
        out_specs=vmem,
        scratch_shapes=[
            V((1, hs), f32), V(states.shape, bf), V((8, hs) if direct else sent.shape, bf),
            V((1, depth), f32), V((G * gh, hs), bf), V((G, hs), bf), V((G, hs), bf),
            V((R, count, columns), bf),
            V((2, Y, X, steps, rows, depth), bf), V((R * count, depth), f32),
            V((R * count, depth), bf), V((count, hs), f32),
            V((N, depth, cw), bf), V((2, N, gq, columns), bf),
            V((rows, G, context, hs), bf), V((rows, G, context, hs), bf),
            V((N, Y, X, count, cw), f32),
            V((N, Y, X, count, cw), bf), V((N, Y, X, count, cw), bf),
            V((N, k1, count, cw), bf), V((N, k1, count, cw), bf),
            V((N, k2, count, cw), bf), V((N, k2, count, cw), bf),
            V((N, count, cw), bf), V((N, count, cw), bf),
            V((G, count, cw), f32), V((G, gh * count, hs), f32),
            V((G, count, hs), bf), V((G, count, hs), bf),
            V((2, gh * steps, context), f32), V((G, gh * count, hs), f32),
            V((G, T, Y, X, count, gq), bf), V((2, half * count, columns), f32),
            V((2, Y, X, count, columns), bf),
            dma((N, 3)), dma((N,)), dma((rows, G)), dma((rows, G)), dma((7,)), dma((R,)), dma((R,)),
            dma((N,)), dma((N,)), dma((N, k1)), dma((N, k1)), dma((N, k2)), dma((N, k2)),
            dma((N,)), dma((N,)),
            dma((G, T)), dma((G, T)), dma((G, T, half)), dma((G, T, half)),
            dma((N,)), dma((N,)), dma((2, half)), dma((R,)), pltpu.SemaphoreType.REGULAR,
        ],
        compiler_params=pltpu.CompilerParams(
            collective_id=0, has_side_effects=True, vmem_limit_bytes=VMEM_KIB << 10
        ),
        name="block",
    )(
        lengths, freqs, states, sent, gain,
        bias_query.reshape(-1, hs), bias_key.reshape(-1, hs), bias_value.reshape(-1, hs),
        w_query, w_key, w_value, w_out, key_cache, value_cache,
    )
    if direct:
        return pieces
    summed = pieces.reshape(R, steps, rows, columns).transpose(1, 2, 0, 3)
    summed = summed.reshape(steps, rows, share).astype(f32)
    residual = lax.dynamic_slice_in_dim(states, t * share, share, 2).astype(f32)
    return (residual + summed).astype(bf)


def solution(mesh):
    return jax.shard_map(
        functools.partial(on_device, mesh.shape["rep"], mesh.shape["tp"]),
        mesh=mesh,
        in_specs=(
            P(None, "rep", None), P(), P(("rep", "tp"), None), P(("rep", "tp"), None),
            P(("rep", "tp"), None), P(None, ("rep", "tp")), P("tp"), P("tp"), P("tp"),
            P("rep", "tp", None, None), P("rep", "tp", None, None), P("rep"),
        ),
        out_specs=P(None, "rep", "tp"),
        check_vma=False,
    )
```

```python
import functools

import jax
import jax.numpy as jnp
import numpy as np
from jax import lax
from jax.experimental import pallas as pl
from jax.experimental.pallas import tpu as pltpu
from jax.sharding import PartitionSpec as P

THETA = 1000000.0
EPS = 1e-06
MESH = pl.DeviceIdType.MESH
BLK = 1024
TILE = 256
VMEM_KIB = 61440
LOG2E = 1.4426950408889634
CONTRACT = (((1,), (1,)), ((), ()))


def remote(src, dst, send, recv, device):
    return pltpu.make_async_remote_copy(
        src_ref=src, dst_ref=dst, send_sem=send, recv_sem=recv,
        device_id=device, device_id_type=MESH,
    )


def flip(index, mask, size):
    result, bit = 0, 1
    while bit < size:
        digit = lax.rem(index // bit, 2)
        result = result + bit * (1 - digit if mask & bit else digit)
        bit *= 2
    return result


def block_kernel(
    R, T, direct,
    len_hbm, freq_hbm, x_hbm, send_hbm, gain_hbm, bq_hbm, bk_hbm, bv_hbm,
    wq_ref, wk_ref, wv_ref, wo_ref, kc_ref, vc_ref,
    out_ref,
    len_ref, freq_ref, x_ref, send_ref, gain_ref, bq_ref, bk_ref, bv_ref, pieces,
    xs, xf, xg, ssq, wbuf, wobuf, kv,
    own, send0, recv0, send1, recv1, send2, recv2, send3, recv3,
    joined, qbuf, knew, vnew, sbuf, abuf, att, acc, obuf,
    isem, wsem, kvsem, wosem, xsend, xrecv, s0s, s0r, s1s, s1r, s2s, s2r, s3s, s3r,
    zsend, zrecv, csend, crecv, fsend, frecv, wsend, wrecv, osend, orecv, ready,
):
    r, t = lax.axis_index("rep"), lax.axis_index("tp")
    half, X = R // 2, 2
    Y = half // X
    c, q = lax.rem(r, 2), r // 2
    x, y = lax.rem(q, X), q // X
    steps, rows, width = x_ref.shape
    count = steps * rows
    depth = wq_ref.shape[0]
    G = kc_ref.shape[1]
    context, hs = kc_ref.shape[2], kc_ref.shape[3]
    gq = wq_ref.shape[1] // (T * G)
    gh = gq // hs
    cw = gq + 2 * hs
    N = G * T
    columns = wo_ref.shape[1]
    bf, f32 = jnp.bfloat16, jnp.float32

    def dev(yy, xx, cc):
        return ((yy * X + xx) * 2 + cc, t)

    partner = dev(y, x, 1 - c)

    def target(j):
        return flip(t, T - 1 - j, T)

    def weights(n):
        g, d = n // T, target(n % T)
        group = []
        for i, (ref, size, place) in enumerate(
            ((wq_ref, gq, 0), (wk_ref, hs, gq), (wv_ref, hs, gq + hs))
        ):
            start = pl.multiple_of((d * G + g) * size, size)
            group.append(
                pltpu.make_async_copy(
                    ref.at[:, pl.ds(start, size)],
                    wbuf.at[n, :, pl.ds(place, size)],
                    wsem.at[n],
                )
            )
        return group

    loads = [weights(n) for n in range(N)]

    barrier = pltpu.get_barrier_semaphore()
    for d in range(1, R):
        pl.semaphore_signal(
            barrier, inc=1, device_id=(lax.rem(r + d, R), t), device_id_type=MESH
        )
    for d in range(1, T):
        pl.semaphore_signal(
            barrier, inc=1, device_id=(r, lax.rem(t + d, T)), device_id_type=MESH
        )
    mine_at = pl.ds(pl.multiple_of((r * T + t) * depth, depth) if direct else 0, depth)
    small = [
        pltpu.make_async_copy(src, dst, isem.at[i])
        for i, (src, dst) in enumerate((
            (x_hbm, x_ref), (gain_hbm.at[:, mine_at], gain_ref), (freq_hbm, freq_ref),
            (bq_hbm, bq_ref), (bk_hbm, bk_ref), (bv_hbm, bv_ref), (len_hbm, len_ref),
            (send_hbm, send_ref),
        ))
        if direct is False or dst is not send_ref
    ]
    for copy in small:
        copy.start()
    small[0].wait()
    if not direct:
        small[-1].wait()
    for group in loads:
        for copy in group:
            copy.start()
    pl.semaphore_wait(barrier, R + T - 2)

    def here(ref, sem):
        pltpu.make_async_copy(ref, ref, sem).wait()

    def sent(ref, sem):
        remote(ref, ref, sem, xrecv, partner).wait_send()

    def got(ref, sem):
        remote(ref, ref, xsend, sem, partner).wait_recv()

    def features(peer):
        if direct:
            start = pl.multiple_of((peer * T + t) * depth, depth)
            return x_ref.at[:, :, pl.ds(start, depth)]
        return send_ref.at[peer]

    def slot_of(peer):
        return xs.at[lax.rem(peer, 2) * half + peer // 2]

    for d in range(1, R):
        peer = lax.rem(r + d, R)
        remote(features(peer), slot_of(r), xsend, xrecv, (peer, t)).start()
    for d in range(1, T):
        pl.semaphore_signal(
            ready, inc=1, device_id=(r, lax.rem(t + d, T)), device_id_type=MESH
        )

    caches = [
        pltpu.make_async_copy(ref.at[b, h], kv.at[i, b, h], kvsem.at[h])
        for h in range(G)
        for b in range(rows)
        for i, ref in enumerate((kc_ref, vc_ref))
    ]
    outs = []
    for k in range(N):
        part = wo_ref.at[pl.ds(k * gq, gq), :]
        outs.append((
            pltpu.make_async_copy(part, wobuf.at[c, k], wosem),
            remote(part, wobuf.at[c, k], wsend, wrecv, partner),
        ))
    for copy in small[1:7]:
        copy.wait()

    for i in range(steps):
        value = x_ref[i].astype(f32)
        square = jnp.sum(value * value, axis=-1, keepdims=True)
        ssq[pl.ds(i * rows, rows), :] = jnp.broadcast_to(square, (rows, hs))
    factor = lax.rsqrt(ssq[...] * (1.0 / width) + EPS)
    rank = lax.broadcasted_iota(jnp.int32, (count, hs), 0)
    spot = lax.broadcasted_iota(jnp.int32, (count, hs), 1)
    position = rank // rows
    for b in range(rows):
        position = position + jnp.where(lax.rem(rank, rows) == b, len_ref[b], 0)
    angle = position.astype(f32) * freq_ref[...]
    cosine = jnp.cos(angle)
    sine = jnp.where(spot < hs // 2, -1.0, 1.0) * jnp.sin(angle)

    got(xs.at[pl.ds(0, R - 1)], xrecv)
    xs[c * half + q] = x_ref[:, :, mine_at] if direct else send_ref[r]
    for k in range(2):
        cc = 1 - c if k == 0 else c
        for yy in range(Y):
            for xx in range(X):
                for i in range(steps):
                    at = (((k * Y + yy) * X + xx) * steps + i) * rows
                    xf[pl.ds(at, rows), :] = xs[cc * half + yy * X + xx, i].astype(f32)
    xg[...] = (xf[...] * gain_ref[...]).astype(bf)

    def stage0(n):
        here(wbuf.at[n], wsem.at[n])
        for i in range(cw // TILE):
            cols = pl.ds(i * TILE, TILE)
            part = jnp.dot(xg[...], wbuf[n, :, cols], preferred_element_type=f32)
            part = part.reshape(2, Y, X, count, TILE)
            send0[n, :, :, :, cols] = part[0].astype(bf)
            own[n, :, :, :, cols] = part[1]
        remote(send0.at[n], recv0.at[n], s0s, s0r.at[n], partner).start()

    def x_first(n):
        return n % 2 == 0

    def stage1(n):
        got(recv0.at[n], s0r.at[n])
        if x_first(n):
            for yy in range(Y):
                send1[n, yy] = (own[n, yy, 1 - x] + recv0[n, yy, 1 - x].astype(f32)).astype(bf)
            piece = pl.ds(0, Y)
            remote(
                send1.at[n, piece], recv1.at[n, piece], s1s.at[0], s1r.at[n], dev(y, 1 - x, c)
            ).start()
            for yy in range(Y):
                own[n, yy, x] += recv0[n, yy, x].astype(f32)
        else:
            for d in range(1, Y):
                yy = lax.rem(y + d, Y)
                piece = pl.ds((d - 1) * X, X)
                send1[n, piece] = (own[n, yy] + recv0[n, yy].astype(f32)).astype(bf)
                remote(
                    send1.at[n, piece], recv1.at[n, piece], s1s.at[1], s1r.at[n], dev(yy, x, c)
                ).start()
            own[n, y] += recv0[n, y].astype(f32)

    def stage2(n):
        if x_first(n):
            got(recv1.at[n, pl.ds(0, Y)], s1r.at[n])
            for d in range(1, Y):
                yy = lax.rem(y + d, Y)
                send2[n, d - 1] = (own[n, yy, x] + recv1[n, yy].astype(f32)).astype(bf)
                remote(
                    send2.at[n, d - 1], recv2.at[n, d - 1], s2s.at[0], s2r.at[n], dev(yy, x, c)
                ).start()
            own[n, y, x] += recv1[n, y].astype(f32)
        else:
            got(recv1.at[n, pl.ds(0, (Y - 1) * X)], s1r.at[n])
            away, keep = own[n, y, 1 - x], own[n, y, x]
            for d in range(1, Y):
                away += recv1[n, (d - 1) * X + 1 - x].astype(f32)
                keep += recv1[n, (d - 1) * X + x].astype(f32)
            send2[n, 0] = away.astype(bf)
            remote(
                send2.at[n, 0], recv2.at[n, 0], s2s.at[1], s2r.at[n], dev(y, 1 - x, c)
            ).start()
            own[n, y, x] = keep

    def stage3(n):
        g, j = n // T, n % T
        total = own[n, y, x]
        pieces_in = Y - 1 if x_first(n) else 1
        got(recv2.at[n, pl.ds(0, pieces_in)], s2r.at[n])
        for d in range(pieces_in):
            total += recv2[n, d].astype(f32)
        if j < T - 1:
            send3[n] = total.astype(bf)
            remote(send3.at[n], recv3.at[n], s3s, s3r.at[g], (r, target(j))).start()
        else:
            joined[g] = total

    def sums_sent():
        part = pl.ds(0, N // 2)
        sent(xs.at[pl.ds(0, R - 1)], xsend)
        sent(send0, s0s)
        sent(send1.at[part, pl.ds(0, Y)], s1s.at[0])
        sent(send1.at[part, pl.ds(0, (Y - 1) * X)], s1s.at[1])
        sent(send2.at[part, pl.ds(0, Y - 1)], s2s.at[0])
        sent(send2.at[part, pl.ds(0, 1)], s2s.at[1])
        sent(send3.at[pl.ds(0, N - G)], s3s)

    def turn(value):
        return value * cosine + pltpu.roll(value, hs // 2, 1) * sine

    def stage4(g):
        got(recv3.at[pl.ds(g * T, T - 1)], s3r.at[g])
        for j in range(T - 1):
            joined[g] += recv3[g * T + j].astype(f32)
        for k in range(gh):
            bias = bq_ref[pl.ds(g * gh + k, 1), :].astype(f32)
            value = joined[g, :, pl.ds(k * hs, hs)] * factor + bias
            qbuf[g, pl.ds(k * count, count), :] = turn(value) * (LOG2E / hs**0.5)
        bias = bk_ref[pl.ds(g, 1), :].astype(f32)
        knew[g] = turn(joined[g, :, pl.ds(gq, hs)] * factor + bias).astype(bf)
        bias = bv_ref[pl.ds(g, 1), :].astype(f32)
        vnew[g] = (joined[g, :, pl.ds(gq + hs, hs)] * factor + bias).astype(bf)

    block = min(BLK, context)
    lines = gh * steps

    def unit(g, b):
        if b == 0:
            here(kv.at[:, :, g], kvsem.at[g])
        length = len_ref[b]
        qb = qbuf[g, pl.ds(b, lines, stride=rows), :].astype(bf)
        fresh = lax.dot_general(qb, knew[g], CONTRACT, preferred_element_type=f32)
        asker = lax.rem(lax.broadcasted_iota(jnp.int32, (lines, count), 0), steps)
        place = lax.broadcasted_iota(jnp.int32, (lines, count), 1)
        fine = (lax.rem(place, rows) == b) & (place // rows <= asker)
        fresh = jnp.where(fine, fresh, -1e30)
        peak = jnp.max(fresh, axis=-1, keepdims=True)
        tops = None
        for k in range(context // block):
            part = pl.ds(k * block, block)
            scores = lax.dot_general(qb, kv[0, b, g, part, :], CONTRACT, preferred_element_type=f32)
            where = k * block + lax.broadcasted_iota(jnp.int32, (lines, block), 1)
            scores = jnp.where(where < length, scores, -1e30)
            sbuf[b % 2, :, part] = scores
            for s in range(block // hs):
                piece = scores[:, s * hs : (s + 1) * hs]
                tops = piece if tops is None else jnp.maximum(tops, piece)
        peak = jnp.maximum(peak, jnp.max(tops, axis=-1, keepdims=True))
        weights = jnp.exp2(fresh - peak)
        total = jnp.sum(weights, axis=-1, keepdims=True)
        result = jnp.dot(weights.astype(bf), vnew[g], preferred_element_type=f32)
        sums = None
        for k in range(context // block):
            part = pl.ds(k * block, block)
            weights = jnp.exp2(sbuf[b % 2, :, part] - peak)
            for s in range(block // hs):
                piece = weights[:, s * hs : (s + 1) * hs]
                sums = piece if sums is None else sums + piece
            result += jnp.dot(
                weights.astype(bf), kv[1, b, g, part, :], preferred_element_type=f32
            )
        total = total + jnp.sum(sums, axis=-1, keepdims=True)
        abuf[g, pl.ds(b, lines, stride=rows), :] = result / total

    def finish(g):
        for k in range(gh):
            att[g, t, q, :, pl.ds(k * hs, hs)] = abuf[g, pl.ds(k * count, count), :].astype(bf)

    def spread(g):
        mine = att.at[g, t, q]
        for m in range(T - 1, 0, -1):
            remote(mine, mine, zsend.at[g], zrecv.at[g, m], (r, flip(t, m, T))).start()
        across(g, 0)

    def across(g, m):
        piece = att.at[g, flip(t, m, T), q]
        if m:
            got(piece, zrecv.at[g, m])
        for e in range(1, half):
            to = lax.rem(q + e, half)
            remote(piece, piece, csend.at[g], crecv.at[g, m], (2 * to + c, t)).start()

    def forward(g):
        got(att.at[g, t, pl.ds(0, half - 1)], crecv.at[g, 0])
        for e in range(1, half):
            piece = att.at[g, t, lax.rem(q + e, half)]
            remote(piece, piece, fsend.at[g], frecv.at[g], (r, flip(t, 1, T))).start()

    def collect(g, m):
        some = att.at[g, flip(t, m, T), pl.ds(0, half - 1)]
        if m == 1:
            got(att.at[g, flip(t, m, T), q], zrecv.at[g, m])
            got(some, frecv.at[g])
        elif m:
            got(some, crecv.at[g, m])

    def rows_sent(g):
        sent(att.at[g, pl.ds(0, T - 1), 0], zsend.at[g])
        sent(att.at[g, pl.ds(0, T - 1), pl.ds(0, half - 1)], csend.at[g])
        sent(att.at[g, 0, pl.ds(0, half - 1)], fsend.at[g])

    def multiply(g, m, first):
        tt = flip(t, m, T)
        lines = att[g, tt].reshape(half * count, gq)
        for k in range(2):
            part = jnp.dot(lines, wobuf[k, tt * G + g], preferred_element_type=f32)
            if first:
                acc[k] = part
            else:
                acc[k] += part

    early = N // 2
    for n in range(early):
        stage0(n)
    for n in range(early):
        stage1(n)
    for n in range(early, N):
        stage0(n)
    for copy in caches:
        copy.start()
    for copy, swap in outs:
        copy.start()
    for n in range(early, min(early + 2, N)):
        stage1(n)
    for p in range(0, N, 2):
        if p >= 4:
            stage3(p - 4)
            stage3(p - 3)
        stage2(p)
        stage2(p + 1)
        if p >= 2 and early + p < N:
            stage1(early + p)
            stage1(early + p + 1)
    for n in range(max(N - 4, 0), N):
        stage3(n)
    for copy, swap in outs:
        swap.start()
    for g in range(G):
        stage4(g)
        for b in range(rows):
            unit(g, b)
        finish(g)
        spread(g)
    for g in range(G):
        for m in range(2, T):
            across(g, m)
        forward(g)
        if g == 0:
            sums_sent()
            here(wobuf.at[c], wosem)
            got(wobuf.at[1 - c], wrecv)
        if g:
            for m in range(T):
                collect(g - 1, m)
                multiply(g - 1, m, g == 1 and m == 0)
    for m in range(T):
        collect(G - 1, m)
        multiply(G - 1, m, G == 1 and m == 0)

    obuf[...] = acc[...].astype(bf).reshape(obuf.shape)
    pl.semaphore_wait(ready, T - 1)
    homes = []
    for k in range(2):
        block_at = (2 * q + k) * T + t
        home, slot = block_at // R, lax.rem(block_at, R)
        for d in range(1, half):
            to = lax.rem(q + d, half)
            remote(
                obuf.at[k * half + to], pieces.at[slot], osend.at[0], orecv, (2 * to + c, home)
            ).start()
        mine = obuf.at[k * half + q]
        stay = pltpu.make_async_copy(mine, pieces.at[slot], orecv)
        go = remote(mine, pieces.at[slot], osend.at[1 + k], orecv, (r, home))
        homes.append((home, go))

        @pl.when(home == t)
        def _():
            stay.start()

        @pl.when(home != t)
        def _():
            go.start()

    for g in range(G):
        rows_sent(g)
    sent(wobuf.at[0], wsend)
    here(pieces, orecv)

    def give(s):
        if direct:
            value = pieces[s].astype(f32)
            cols = pl.ds(s * columns, columns)
            from_x = pl.ds(pl.multiple_of(t * R * columns + s * columns, columns), columns)
            for i in range(steps):
                out_ref[i, :, cols] = (
                    x_ref[i, :, from_x].astype(f32) + value[i * rows : (i + 1) * rows]
                ).astype(bf)
        else:
            out_ref[s] = pieces[s]

    for s in range(R):
        give(s)
    sent(obuf.at[pl.ds(0, 2 * (half - 1))], osend.at[0])
    for home, go in homes:
        @pl.when(home != t)
        def _(go=go):
            go.wait_send()


def on_device(
    R, T, states, norm_gain, w_query, w_key, w_value, w_out,
    bias_query, bias_key, bias_value, key_cache, value_cache, lengths,
):
    steps, rows, width = states.shape
    G, context, hs = key_cache.shape[1:]
    count = steps * rows
    depth = w_query.shape[0]
    columns = w_out.shape[1]
    gq = w_query.shape[1] // (T * G)
    gh = gq // hs
    cw = gq + 2 * hs
    N = G * T
    half, X = R // 2, 2
    Y = half // X
    direct = depth % hs == 0 and columns % hs == 0
    share = R * columns
    t = lax.axis_index("tp")
    at = lax.axis_index("rep") * T + t
    bf, f32 = jnp.bfloat16, jnp.float32
    gain = norm_gain.reshape(1, width)
    sent = states
    if not direct:
        gain = lax.dynamic_slice_in_dim(gain, at * depth, depth, 1)
        sent = states.reshape(steps, rows, R, T, depth)
        sent = lax.dynamic_index_in_dim(sent, t, 3, keepdims=False).transpose(2, 0, 1, 3)
    result = (steps, rows, share) if direct else (R, count, columns)
    lane = np.arange(hs) % (hs // 2)
    freqs = (np.float32(THETA) ** (-lane.astype(np.float32) * np.float32(2.0) / np.float32(hs)))
    freqs = jnp.asarray(freqs.astype(np.float32).reshape(1, hs))
    vmem = pl.BlockSpec(memory_space=pltpu.VMEM)
    hbm = pl.BlockSpec(memory_space=pltpu.HBM)
    dma = pltpu.SemaphoreType.DMA
    V = pltpu.VMEM
    k1, k2 = max(Y, (Y - 1) * X), max(Y - 1, 1)
    pieces = pl.pallas_call(
        functools.partial(block_kernel, R, T, direct),
        out_shape=pltpu.VMEM(result, bf),
        in_specs=[hbm] * 14,
        out_specs=vmem,
        scratch_shapes=[
            pltpu.SMEM((rows,), jnp.int32), V((1, hs), f32), V(states.shape, bf), V((8, hs) if direct else sent.shape, bf),
            V((1, depth), f32), V((G * gh, hs), bf), V((G, hs), bf), V((G, hs), bf),
            V((R, count, columns), bf),
            V((R, steps, rows, depth), bf), V((R * count, depth), f32),
            V((R * count, depth), bf), V((count, hs), f32),
            V((N, depth, cw), bf), V((2, N, gq, columns), bf),
            V((2, rows, G, context, hs), bf),
            V((N, Y, X, count, cw), f32),
            V((N, Y, X, count, cw), bf), V((N, Y, X, count, cw), bf),
            V((N, k1, count, cw), bf), V((N, k1, count, cw), bf),
            V((N, k2, count, cw), bf), V((N, k2, count, cw), bf),
            V((N, count, cw), bf), V((N, count, cw), bf),
            V((G, count, cw), f32), V((G, gh * count, hs), f32),
            V((G, count, hs), bf), V((G, count, hs), bf),
            V((2, gh * steps, context), f32), V((G, gh * count, hs), f32),
            V((G, T, half, count, gq), bf), V((2, half * count, columns), f32),
            V((2 * half, count, columns), bf),
            dma((8,)), dma((N,)), dma((G,)), dma, dma, dma, dma, dma((N,)), dma((2,)), dma((N,)),
            dma((2,)), dma((N,)), dma, dma((G,)),
            dma((G,)), dma((G, T)), dma((G,)), dma((G, T)), dma((G,)), dma((G,)), dma, dma,
            dma((3,)), dma, pltpu.SemaphoreType.REGULAR,
        ],
        compiler_params=pltpu.CompilerParams(
            collective_id=0, has_side_effects=True, vmem_limit_bytes=VMEM_KIB << 10
        ),
        name="block",
    )(
        *(
            pltpu.with_memory_space_constraint(value, pltpu.HBM)
            for value in (
                lengths, freqs, states, sent, gain,
                bias_query.reshape(-1, hs), bias_key.reshape(-1, hs), bias_value.reshape(-1, hs),
                w_query, w_key, w_value, w_out, key_cache, value_cache,
            )
        )
    )
    if direct:
        return pieces
    summed = pieces.reshape(R, steps, rows, columns).transpose(1, 2, 0, 3)
    summed = summed.reshape(steps, rows, share).astype(f32)
    residual = lax.dynamic_slice_in_dim(states, t * share, share, 2).astype(f32)
    return (residual + summed).astype(bf)


def solution(mesh):
    return jax.shard_map(
        functools.partial(on_device, mesh.shape["rep"], mesh.shape["tp"]),
        mesh=mesh,
        in_specs=(
            P(None, "rep", None), P(), P(("rep", "tp"), None), P(("rep", "tp"), None),
            P(("rep", "tp"), None), P(None, ("rep", "tp")), P("tp"), P("tp"), P("tp"),
            P("rep", "tp", None, None), P("rep", "tp", None, None), P("rep"),
        ),
        out_specs=P(None, "rep", "tp"),
        check_vma=False,
    )
```

```python
import functools

import jax
import jax.numpy as jnp
import numpy as np
from jax import lax
from jax.experimental import pallas as pl
from jax.experimental.pallas import tpu as pltpu
from jax.sharding import PartitionSpec as P

THETA = 1000000.0
EPS = 1e-06
MESH = pl.DeviceIdType.MESH
BLK = 2048
TILE = 256
VMEM_KIB = 61440
LOG2E = 1.4426950408889634
CONTRACT = (((1,), (1,)), ((), ()))


def remote(src, dst, send, recv, device):
    return pltpu.make_async_remote_copy(
        src_ref=src, dst_ref=dst, send_sem=send, recv_sem=recv,
        device_id=device, device_id_type=MESH,
    )


def flip(index, mask, size):
    result, bit = 0, 1
    while bit < size:
        digit = lax.rem(index // bit, 2)
        result = result + bit * (1 - digit if mask & bit else digit)
        bit *= 2
    return result


def block_kernel(
    R, T, direct,
    len_hbm, freq_hbm, x_hbm, send_hbm, gain_hbm, bq_hbm, bk_hbm, bv_hbm,
    wq_ref, wk_ref, wv_ref, wo_ref, kc_ref, vc_ref,
    out_ref,
    len_ref, freq_ref, x_ref, send_ref, gain_ref, bq_ref, bk_ref, bv_ref, pieces,
    xs, xf, xg, ssq, wbuf, wobuf, kv,
    own, send0, recv0, send1, recv1, send2, recv2, send3, recv3,
    joined, qbuf, knew, vnew, sbuf, abuf, att, acc, obuf,
    isem, wsem, kvsem, wosem, xsend, xrecv, s0s, s0r, s1s, s1r, s2s, s2r, s3s, s3r,
    zsend, zrecv, csend, crecv, fsend, frecv, wsend, wrecv, osend, orecv, ready,
):
    r, t = lax.axis_index("rep"), lax.axis_index("tp")
    half, X = R // 2, 2
    Y = half // X
    c, q = lax.rem(r, 2), r // 2
    x, y = lax.rem(q, X), q // X
    steps, rows, width = x_ref.shape
    count = steps * rows
    depth = wq_ref.shape[0]
    G = kc_ref.shape[1]
    context, hs = kc_ref.shape[2], kc_ref.shape[3]
    gq = wq_ref.shape[1] // (T * G)
    gh = gq // hs
    cw = gq + 2 * hs
    N = G * T
    columns = wo_ref.shape[1]
    bf, f32 = jnp.bfloat16, jnp.float32

    def dev(yy, xx, cc):
        return ((yy * X + xx) * 2 + cc, t)

    partner = dev(y, x, 1 - c)

    def target(j):
        return flip(t, T - 1 - j, T)

    def weights(n):
        g, d = n // T, target(n % T)
        group = []
        for i, (ref, size, place) in enumerate(
            ((wq_ref, gq, 0), (wk_ref, hs, gq), (wv_ref, hs, gq + hs))
        ):
            start = pl.multiple_of((d * G + g) * size, size)
            group.append(
                pltpu.make_async_copy(
                    ref.at[:, pl.ds(start, size)],
                    wbuf.at[n, :, pl.ds(place, size)],
                    wsem.at[n],
                )
            )
        return group

    loads = [weights(n) for n in range(N)]

    barrier = pltpu.get_barrier_semaphore()
    for d in range(1, R):
        pl.semaphore_signal(
            barrier, inc=1, device_id=(lax.rem(r + d, R), t), device_id_type=MESH
        )
    for d in range(1, T):
        pl.semaphore_signal(
            barrier, inc=1, device_id=(r, lax.rem(t + d, T)), device_id_type=MESH
        )
    mine_at = pl.ds(pl.multiple_of((r * T + t) * depth, depth) if direct else 0, depth)
    small = [
        pltpu.make_async_copy(src, dst, isem.at[i])
        for i, (src, dst) in enumerate((
            (x_hbm, x_ref), (gain_hbm.at[:, mine_at], gain_ref), (freq_hbm, freq_ref),
            (bq_hbm, bq_ref), (bk_hbm, bk_ref), (bv_hbm, bv_ref), (len_hbm, len_ref),
            (send_hbm, send_ref),
        ))
        if direct is False or dst is not send_ref
    ]
    for copy in small:
        copy.start()
    small[0].wait()
    if not direct:
        small[-1].wait()
    for group in loads:
        for copy in group:
            copy.start()
    pl.semaphore_wait(barrier, R + T - 2)

    def here(ref, sem):
        pltpu.make_async_copy(ref, ref, sem).wait()

    def sent(ref, sem):
        remote(ref, ref, sem, xrecv, partner).wait_send()

    def got(ref, sem):
        remote(ref, ref, xsend, sem, partner).wait_recv()

    def features(peer):
        if direct:
            start = pl.multiple_of((peer * T + t) * depth, depth)
            return x_ref.at[:, :, pl.ds(start, depth)]
        return send_ref.at[peer]

    def slot_of(peer):
        return xs.at[lax.rem(peer, 2) * half + peer // 2]

    for d in range(1, R):
        peer = lax.rem(r + d, R)
        remote(features(peer), slot_of(r), xsend, xrecv, (peer, t)).start()
    for d in range(1, T):
        pl.semaphore_signal(
            ready, inc=1, device_id=(r, lax.rem(t + d, T)), device_id_type=MESH
        )

    caches = [
        pltpu.make_async_copy(ref.at[b, h], kv.at[i, b, h], kvsem.at[h])
        for h in range(G)
        for b in range(rows)
        for i, ref in enumerate((kc_ref, vc_ref))
    ]
    outs = []
    for k in range(N):
        part = wo_ref.at[pl.ds(k * gq, gq), :]
        outs.append((
            pltpu.make_async_copy(part, wobuf.at[c, k], wosem),
            remote(part, wobuf.at[c, k], wsend, wrecv, partner),
        ))
    for copy in small[1:7]:
        copy.wait()

    for i in range(steps):
        value = x_ref[i].astype(f32)
        square = jnp.sum(value * value, axis=-1, keepdims=True)
        ssq[pl.ds(i * rows, rows), :] = jnp.broadcast_to(square, (rows, hs))
    factor = lax.rsqrt(ssq[...] * (1.0 / width) + EPS)
    rank = lax.broadcasted_iota(jnp.int32, (count, hs), 0)
    spot = lax.broadcasted_iota(jnp.int32, (count, hs), 1)
    position = rank // rows
    for b in range(rows):
        position = position + jnp.where(lax.rem(rank, rows) == b, len_ref[b], 0)
    angle = position.astype(f32) * freq_ref[...]
    cosine = jnp.cos(angle)
    sine = jnp.where(spot < hs // 2, -1.0, 1.0) * jnp.sin(angle)

    got(xs.at[pl.ds(0, R - 1)], xrecv)
    xs[c * half + q] = x_ref[:, :, mine_at] if direct else send_ref[r]
    for k in range(2):
        cc = 1 - c if k == 0 else c
        for yy in range(Y):
            for xx in range(X):
                for i in range(steps):
                    at = (((k * Y + yy) * X + xx) * steps + i) * rows
                    xf[pl.ds(at, rows), :] = xs[cc * half + yy * X + xx, i].astype(f32)
    xg[...] = (xf[...] * gain_ref[...]).astype(bf)

    def stage0(n):
        here(wbuf.at[n], wsem.at[n])
        for i in range(cw // TILE):
            cols = pl.ds(i * TILE, TILE)
            part = jnp.dot(xg[...], wbuf[n, :, cols], preferred_element_type=f32)
            part = part.reshape(2, Y, X, count, TILE)
            send0[n, :, :, :, cols] = part[0].astype(bf)
            own[n, :, :, :, cols] = part[1]
        remote(send0.at[n], recv0.at[n], s0s, s0r.at[n], partner).start()

    def x_first(n):
        return n % 2 == 0

    def stage1(n):
        got(recv0.at[n], s0r.at[n])
        if x_first(n):
            for yy in range(Y):
                send1[n, yy] = (own[n, yy, 1 - x] + recv0[n, yy, 1 - x].astype(f32)).astype(bf)
            piece = pl.ds(0, Y)
            remote(
                send1.at[n, piece], recv1.at[n, piece], s1s.at[0], s1r.at[n], dev(y, 1 - x, c)
            ).start()
            for yy in range(Y):
                own[n, yy, x] += recv0[n, yy, x].astype(f32)
        else:
            for d in range(1, Y):
                yy = lax.rem(y + d, Y)
                piece = pl.ds((d - 1) * X, X)
                send1[n, piece] = (own[n, yy] + recv0[n, yy].astype(f32)).astype(bf)
                remote(
                    send1.at[n, piece], recv1.at[n, piece], s1s.at[1], s1r.at[n], dev(yy, x, c)
                ).start()
            own[n, y] += recv0[n, y].astype(f32)

    def stage2(n):
        if x_first(n):
            got(recv1.at[n, pl.ds(0, Y)], s1r.at[n])
            for d in range(1, Y):
                yy = lax.rem(y + d, Y)
                send2[n, d - 1] = (own[n, yy, x] + recv1[n, yy].astype(f32)).astype(bf)
                remote(
                    send2.at[n, d - 1], recv2.at[n, d - 1], s2s.at[0], s2r.at[n], dev(yy, x, c)
                ).start()
            own[n, y, x] += recv1[n, y].astype(f32)
        else:
            got(recv1.at[n, pl.ds(0, (Y - 1) * X)], s1r.at[n])
            away, keep = own[n, y, 1 - x], own[n, y, x]
            for d in range(1, Y):
                away += recv1[n, (d - 1) * X + 1 - x].astype(f32)
                keep += recv1[n, (d - 1) * X + x].astype(f32)
            send2[n, 0] = away.astype(bf)
            remote(
                send2.at[n, 0], recv2.at[n, 0], s2s.at[1], s2r.at[n], dev(y, 1 - x, c)
            ).start()
            own[n, y, x] = keep

    def stage3(n):
        g, j = n // T, n % T
        total = own[n, y, x]
        pieces_in = Y - 1 if x_first(n) else 1
        got(recv2.at[n, pl.ds(0, pieces_in)], s2r.at[n])
        for d in range(pieces_in):
            total += recv2[n, d].astype(f32)
        if j < T - 1:
            send3[n] = total.astype(bf)
            remote(send3.at[n], recv3.at[n], s3s, s3r.at[g], (r, target(j))).start()
        else:
            joined[g] = total

    def sums_sent():
        part = pl.ds(0, N // 2)
        sent(xs.at[pl.ds(0, R - 1)], xsend)
        sent(send0, s0s)
        sent(send1.at[part, pl.ds(0, Y)], s1s.at[0])
        sent(send1.at[part, pl.ds(0, (Y - 1) * X)], s1s.at[1])
        sent(send2.at[part, pl.ds(0, Y - 1)], s2s.at[0])
        sent(send2.at[part, pl.ds(0, 1)], s2s.at[1])
        sent(send3.at[pl.ds(0, N - G)], s3s)

    def turn(value):
        return value * cosine + pltpu.roll(value, hs // 2, 1) * sine

    def stage4(g):
        got(recv3.at[pl.ds(g * T, T - 1)], s3r.at[g])
        for j in range(T - 1):
            joined[g] += recv3[g * T + j].astype(f32)
        for k in range(gh):
            bias = bq_ref[pl.ds(g * gh + k, 1), :].astype(f32)
            value = joined[g, :, pl.ds(k * hs, hs)] * factor + bias
            qbuf[g, pl.ds(k * count, count), :] = turn(value) * (LOG2E / hs**0.5)
        bias = bk_ref[pl.ds(g, 1), :].astype(f32)
        knew[g] = turn(joined[g, :, pl.ds(gq, hs)] * factor + bias).astype(bf)
        bias = bv_ref[pl.ds(g, 1), :].astype(f32)
        vnew[g] = (joined[g, :, pl.ds(gq + hs, hs)] * factor + bias).astype(bf)

    block = min(BLK, context)
    lines = gh * steps

    def begin(g, b):
        qb = qbuf[g, pl.ds(b, lines, stride=rows), :].astype(bf)
        fresh = lax.dot_general(qb, knew[g], CONTRACT, preferred_element_type=f32)
        asker = lax.rem(lax.broadcasted_iota(jnp.int32, (lines, count), 0), steps)
        place = lax.broadcasted_iota(jnp.int32, (lines, count), 1)
        fine = (lax.rem(place, rows) == b) & (place // rows <= asker)
        return {"g": g, "b": b, "q": qb, "fresh": jnp.where(fine, fresh, -1e30)}

    def score(u, k):
        g, b, part = u["g"], u["b"], pl.ds(k * block, block)
        scores = lax.dot_general(
            u["q"], kv[0, b, g, part, :], CONTRACT, preferred_element_type=f32
        )
        where = k * block + lax.broadcasted_iota(jnp.int32, (lines, block), 1)
        scores = jnp.where(where < len_ref[b], scores, -1e30)
        sbuf[b % 2, :, part] = scores
        for s in range(block // hs):
            piece = scores[:, s * hs : (s + 1) * hs]
            u["tops"] = jnp.maximum(u["tops"], piece) if "tops" in u else piece

    def settle(u):
        peak = jnp.max(u["fresh"], axis=-1, keepdims=True)
        u["peak"] = jnp.maximum(peak, jnp.max(u["tops"], axis=-1, keepdims=True))
        weights = jnp.exp2(u["fresh"] - u["peak"])
        u["total"] = jnp.sum(weights, axis=-1, keepdims=True)
        u["result"] = jnp.dot(weights.astype(bf), vnew[u["g"]], preferred_element_type=f32)

    def weigh(u, k):
        g, b, part = u["g"], u["b"], pl.ds(k * block, block)
        weights = jnp.exp2(sbuf[b % 2, :, part] - u["peak"])
        for s in range(block // hs):
            piece = weights[:, s * hs : (s + 1) * hs]
            u["sums"] = u["sums"] + piece if "sums" in u else piece
        u["result"] += jnp.dot(
            weights.astype(bf), kv[1, b, g, part, :], preferred_element_type=f32
        )

    def attend(g):
        here(kv.at[:, :, g], kvsem.at[g])
        blocks = range(context // block)
        now = begin(g, 0)
        for k in blocks:
            score(now, k)
        for b in range(rows):
            later = begin(g, b + 1) if b < rows - 1 else None
            settle(now)
            for k in blocks:
                if later:
                    score(later, k)
                weigh(now, k)
            total = now["total"] + jnp.sum(now["sums"], axis=-1, keepdims=True)
            abuf[g, pl.ds(b, lines, stride=rows), :] = now["result"] / total
            now = later

    def finish(g):
        for k in range(gh):
            att[g, t, q, :, pl.ds(k * hs, hs)] = abuf[g, pl.ds(k * count, count), :].astype(bf)

    def spread(g):
        mine = att.at[g, t, q]
        for m in range(T - 1, 0, -1):
            remote(mine, mine, zsend.at[g], zrecv.at[g, m], (r, flip(t, m, T))).start()
        across(g, 0)

    def across(g, m):
        piece = att.at[g, flip(t, m, T), q]
        if m:
            got(piece, zrecv.at[g, m])
        for e in range(1, half):
            to = lax.rem(q + e, half)
            remote(piece, piece, csend.at[g], crecv.at[g, m], (2 * to + c, t)).start()

    def forward(g):
        got(att.at[g, t, pl.ds(0, half - 1)], crecv.at[g, 0])
        for e in range(1, half):
            piece = att.at[g, t, lax.rem(q + e, half)]
            remote(piece, piece, fsend.at[g], frecv.at[g], (r, flip(t, 1, T))).start()

    def collect(g, m):
        some = att.at[g, flip(t, m, T), pl.ds(0, half - 1)]
        if m == 1:
            got(att.at[g, flip(t, m, T), q], zrecv.at[g, m])
            got(some, frecv.at[g])
        elif m:
            got(some, crecv.at[g, m])

    def rows_sent(g):
        sent(att.at[g, pl.ds(0, T - 1), 0], zsend.at[g])
        sent(att.at[g, pl.ds(0, T - 1), pl.ds(0, half - 1)], csend.at[g])
        sent(att.at[g, 0, pl.ds(0, half - 1)], fsend.at[g])

    def multiply(g, m, first):
        tt = flip(t, m, T)
        lines = att[g, tt].reshape(half * count, gq)
        for k in range(2):
            part = jnp.dot(lines, wobuf[k, tt * G + g], preferred_element_type=f32)
            if first:
                acc[k] = part
            else:
                acc[k] += part

    early = N // 2
    for n in range(early):
        stage0(n)
    for n in range(early):
        stage1(n)
    for n in range(early, N):
        stage0(n)
    for copy in caches:
        copy.start()
    for copy, swap in outs:
        copy.start()
    for n in range(early, min(early + 2, N)):
        stage1(n)
    for p in range(0, N, 2):
        if p >= 4:
            stage3(p - 4)
            stage3(p - 3)
        stage2(p)
        stage2(p + 1)
        if p >= 2 and early + p < N:
            stage1(early + p)
            stage1(early + p + 1)
    for n in range(max(N - 4, 0), N):
        stage3(n)
    for copy, swap in outs:
        swap.start()
    for g in range(G):
        stage4(g)
        attend(g)
        finish(g)
        spread(g)
    for g in range(G):
        forward(g)
        for m in range(2, T):
            across(g, m)
        if g == 0:
            sums_sent()
            here(wobuf.at[c], wosem)
            got(wobuf.at[1 - c], wrecv)
        if g:
            for m in range(T):
                collect(g - 1, m)
                multiply(g - 1, m, g == 1 and m == 0)
    for m in range(T):
        collect(G - 1, m)
        multiply(G - 1, m, G == 1 and m == 0)

    obuf[...] = acc[...].astype(bf).reshape(obuf.shape)
    pl.semaphore_wait(ready, T - 1)
    homes = []
    for k in range(2):
        block_at = (2 * q + k) * T + t
        home, slot = block_at // R, lax.rem(block_at, R)
        for d in range(1, half):
            to = lax.rem(q + d, half)
            remote(
                obuf.at[k * half + to], pieces.at[slot], osend.at[0], orecv, (2 * to + c, home)
            ).start()
        mine = obuf.at[k * half + q]
        stay = pltpu.make_async_copy(mine, pieces.at[slot], orecv)
        go = remote(mine, pieces.at[slot], osend.at[1 + k], orecv, (r, home))
        homes.append((home, go))

        @pl.when(home == t)
        def _():
            stay.start()

        @pl.when(home != t)
        def _():
            go.start()

    for g in range(G):
        rows_sent(g)
    sent(wobuf.at[0], wsend)
    here(pieces, orecv)

    def give(s):
        if direct:
            value = pieces[s].astype(f32)
            cols = pl.ds(s * columns, columns)
            from_x = pl.ds(pl.multiple_of(t * R * columns + s * columns, columns), columns)
            for i in range(steps):
                out_ref[i, :, cols] = (
                    x_ref[i, :, from_x].astype(f32) + value[i * rows : (i + 1) * rows]
                ).astype(bf)
        else:
            out_ref[s] = pieces[s]

    for s in range(R):
        give(s)
    sent(obuf.at[pl.ds(0, 2 * (half - 1))], osend.at[0])
    for home, go in homes:
        @pl.when(home != t)
        def _(go=go):
            go.wait_send()


def on_device(
    R, T, states, norm_gain, w_query, w_key, w_value, w_out,
    bias_query, bias_key, bias_value, key_cache, value_cache, lengths,
):
    steps, rows, width = states.shape
    G, context, hs = key_cache.shape[1:]
    count = steps * rows
    depth = w_query.shape[0]
    columns = w_out.shape[1]
    gq = w_query.shape[1] // (T * G)
    gh = gq // hs
    cw = gq + 2 * hs
    N = G * T
    half, X = R // 2, 2
    Y = half // X
    direct = depth % hs == 0 and columns % hs == 0
    share = R * columns
    t = lax.axis_index("tp")
    at = lax.axis_index("rep") * T + t
    bf, f32 = jnp.bfloat16, jnp.float32
    gain = norm_gain.reshape(1, width)
    sent = states
    if not direct:
        gain = lax.dynamic_slice_in_dim(gain, at * depth, depth, 1)
        sent = states.reshape(steps, rows, R, T, depth)
        sent = lax.dynamic_index_in_dim(sent, t, 3, keepdims=False).transpose(2, 0, 1, 3)
    result = (steps, rows, share) if direct else (R, count, columns)
    lane = np.arange(hs) % (hs // 2)
    freqs = (np.float32(THETA) ** (-lane.astype(np.float32) * np.float32(2.0) / np.float32(hs)))
    freqs = jnp.asarray(freqs.astype(np.float32).reshape(1, hs))
    vmem = pl.BlockSpec(memory_space=pltpu.VMEM)
    hbm = pl.BlockSpec(memory_space=pltpu.HBM)
    dma = pltpu.SemaphoreType.DMA
    V = pltpu.VMEM
    k1, k2 = max(Y, (Y - 1) * X), max(Y - 1, 1)
    pieces = pl.pallas_call(
        functools.partial(block_kernel, R, T, direct),
        out_shape=pltpu.VMEM(result, bf),
        in_specs=[hbm] * 14,
        out_specs=vmem,
        scratch_shapes=[
            pltpu.SMEM((rows,), jnp.int32), V((1, hs), f32), V(states.shape, bf), V((8, hs) if direct else sent.shape, bf),
            V((1, depth), f32), V((G * gh, hs), bf), V((G, hs), bf), V((G, hs), bf),
            V((R, count, columns), bf),
            V((R, steps, rows, depth), bf), V((R * count, depth), f32),
            V((R * count, depth), bf), V((count, hs), f32),
            V((N, depth, cw), bf), V((2, N, gq, columns), bf),
            V((2, rows, G, context, hs), bf),
            V((N, Y, X, count, cw), f32),
            V((N, Y, X, count, cw), bf), V((N, Y, X, count, cw), bf),
            V((N, k1, count, cw), bf), V((N, k1, count, cw), bf),
            V((N, k2, count, cw), bf), V((N, k2, count, cw), bf),
            V((N, count, cw), bf), V((N, count, cw), bf),
            V((G, count, cw), f32), V((G, gh * count, hs), f32),
            V((G, count, hs), bf), V((G, count, hs), bf),
            V((2, gh * steps, context), f32), V((G, gh * count, hs), f32),
            V((G, T, half, count, gq), bf), V((2, half * count, columns), f32),
            V((2 * half, count, columns), bf),
            dma((8,)), dma((N,)), dma((G,)), dma, dma, dma, dma, dma((N,)), dma((2,)), dma((N,)),
            dma((2,)), dma((N,)), dma, dma((G,)),
            dma((G,)), dma((G, T)), dma((G,)), dma((G, T)), dma((G,)), dma((G,)), dma, dma,
            dma((3,)), dma, pltpu.SemaphoreType.REGULAR,
        ],
        compiler_params=pltpu.CompilerParams(
            collective_id=0, has_side_effects=True, vmem_limit_bytes=VMEM_KIB << 10
        ),
        name="block",
    )(
        *(
            pltpu.with_memory_space_constraint(value, pltpu.HBM)
            for value in (
                lengths, freqs, states, sent, gain,
                bias_query.reshape(-1, hs), bias_key.reshape(-1, hs), bias_value.reshape(-1, hs),
                w_query, w_key, w_value, w_out, key_cache, value_cache,
            )
        )
    )
    if direct:
        return pieces
    summed = pieces.reshape(R, steps, rows, columns).transpose(1, 2, 0, 3)
    summed = summed.reshape(steps, rows, share).astype(f32)
    residual = lax.dynamic_slice_in_dim(states, t * share, share, 2).astype(f32)
    return (residual + summed).astype(bf)


def solution(mesh):
    return jax.shard_map(
        functools.partial(on_device, mesh.shape["rep"], mesh.shape["tp"]),
        mesh=mesh,
        in_specs=(
            P(None, "rep", None), P(), P(("rep", "tp"), None), P(("rep", "tp"), None),
            P(("rep", "tp"), None), P(None, ("rep", "tp")), P("tp"), P("tp"), P("tp"),
            P("rep", "tp", None, None), P("rep", "tp", None, None), P("rep"),
        ),
        out_specs=P(None, "rep", "tp"),
        check_vma=False,
    )
```
